32 devices in a mesh: heads: 4 (over y, core), tokens: 4 (over z), cols: 2 (over x).
Axes of the slice: x: 2, y: 2, z: 4, core: 2. Of those that a mesh axis runs over, the one named last changes fastest.
Arguments:
- query_in: bfloat16 [2048, 8192], P('tokens', ('heads', 'cols')), may hold values from -24 to 24
- key_in: bfloat16 [2048, 8192], P('tokens', ('heads', 'cols')), may hold values from -24 to 24
- value_in: bfloat16 [2048, 8192], P('tokens', ('heads', 'cols')), may hold values from -6 to 6
- out_grads: bfloat16 [2048, 8192], P('tokens', ('heads', 'cols')), may hold values from -6 to 6
- doc_starts: int32 [6], replicated, may hold values from 0 to 2047, as said below
Outputs:
- input_factor: float32 [8192, 8192], P('heads', ('tokens', 'cols'))
- grad_factor: float32 [8192, 8192], P('heads', ('tokens', 'cols'))
The draws below stay inside these ranges and needn't reach their ends.
Inputs may be any that keep to these rules, and one draw needn't show every extreme that they name: Strictly increasing with the first entry 0; document d runs from doc_starts[d] to the next start (the last one to 2048) - 1. One document holds (4 // 2 + 1) * 512 tokens.
All inputs are finite; a program needn't handle non-finite values.
Results may differ from the reference program's by a relative error of at most 0.0041.
Values may be sent and summed in bfloat16 or wider, within the bound.
A program may use at most 128 MiB of HBM per device.

```python
import math
import jax
import jax.numpy as jnp
from jax import lax

HEAD_DIM = 128
TOK_DEV = 512
DOCS = 6
D = 8192
TOKENS = 2048


def cut_points(key):
    long_len = (TOKENS // TOK_DEV // 2 + 1) * TOK_DEV
    rest_len = TOKENS - long_len
    cut_picks = jax.random.permutation(jax.random.fold_in(key, 11), rest_len - 1)[:DOCS - 2] + 1
    bounds = jnp.concatenate([jnp.zeros((1,), jnp.int32), jnp.sort(cut_picks).astype(jnp.int32), jnp.full((1,), rest_len, jnp.int32)])
    others = bounds[1:] - bounds[:-1]
    long_slot = jax.random.randint(jax.random.fold_in(key, 13), (), 0, DOCS).astype(jnp.int32)
    slots = jnp.arange(DOCS, dtype=jnp.int32)
    other_index = jnp.clip(slots - (slots > long_slot).astype(jnp.int32), 0, DOCS - 2)
    doc_lengths = jnp.where(slots == long_slot, long_len, others[other_index]).astype(jnp.int32)
    return jnp.concatenate([jnp.zeros((1,), jnp.int32), jnp.cumsum(doc_lengths)[:-1].astype(jnp.int32)])


def draw_doc_starts(key, part):
    return cut_points(key)


def background(key, salt):
    return jnp.clip(jax.random.normal(jax.random.fold_in(key, salt), (TOKENS, D), jnp.float32), -4.0, 4.0)


def draw_key_in(key, part):
    result = background(key, 31)
    return result.astype(jnp.bfloat16)


def draw_query_in(key, part):
    result = background(key, 37)
    return result.astype(jnp.bfloat16)


def shard_levels(stream_key, extent, cuts, smallest, largest):
    def one(axis_at, blocks):
        draws = jax.random.uniform(jax.random.fold_in(jax.random.fold_in(stream_key, 6), axis_at), (blocks,), jnp.float32, smallest / len(cuts), largest / len(cuts))
        return jnp.repeat(jnp.exp(draws), extent[axis_at] // blocks).reshape((-1,) + (1,) * (len(extent) - axis_at - 1))

    loudness = one(*cuts[0])
    for cut in cuts[1:]:
        loudness = loudness * one(*cut)
    return loudness


def gaussian(own_key, shape, scale, limit, shards=(), kind=jnp.bfloat16):
    factor_of = shard_levels(own_key, shape, shards, -0.22, 0.18) if shards else 1.0
    values = jax.random.normal(own_key, shape, jnp.float32) * scale * factor_of
    return jnp.minimum(jnp.maximum(values, -limit), limit).astype(kind)


def setup_inputs(seed: int = 0) -> dict:
    seeds = jax.random.split(jax.random.key(seed), 6)
    return {
        "query_in": draw_query_in(jax.random.fold_in(seeds[5], 71), 0),
        "key_in": draw_key_in(jax.random.fold_in(seeds[5], 71), 0),
        "value_in": gaussian(seeds[2], (TOKENS, D), 1.0, 6.0, ((0, 4), (1, 8))),
        "out_grads": gaussian(seeds[3], (TOKENS, D), 1.0, 6.0, ((0, 4), (1, 8))),
        "doc_starts": draw_doc_starts(jax.random.fold_in(seeds[5], 71), 0),
    }


MASK_FLOOR = -1e+30

def document_ids(positions, doc_starts):
    return lax.optimization_barrier(jnp.sum((positions[:, None] >= doc_starts[None, :]).astype(jnp.int32), axis=1)) - 1

def reference(query_in, key_in, value_in, out_grads, doc_starts):
    all_tokens, row_width = query_in.shape
    head_count = row_width // HEAD_DIM
    positions = jnp.arange(all_tokens, dtype=jnp.int32)
    doc_ids = document_ids(positions, doc_starts)
    allowed = doc_ids[:, None] == doc_ids[None, :]
    score_scale = 1.0 / math.sqrt(HEAD_DIM)

    def per_head(head_index):
        col_begin = (head_index * HEAD_DIM).astype(jnp.int32)

        def select_cols(source):
            return lax.dynamic_slice_in_dim(source, col_begin, HEAD_DIM, 1).astype(jnp.float32)
        scores = jnp.dot(select_cols(query_in), select_cols(key_in).T, precision=lax.Precision.HIGHEST) * score_scale
        masked = jnp.where(allowed, scores, MASK_FLOOR)
        row_peak = lax.optimization_barrier(jnp.max(masked, axis=1))
        row_mass = lax.optimization_barrier(jnp.sum(jnp.where(allowed, jnp.exp(masked - row_peak[:, None]), 0.0), axis=1))
        log_total = row_peak + jnp.log(row_mass)
        weights = jnp.where(allowed, jnp.exp(scores - log_total[:, None]), 0.0).astype(jnp.bfloat16)
        weights = lax.optimization_barrier(weights).astype(jnp.float32)
        attended = jnp.dot(weights, select_cols(value_in), precision=lax.Precision.HIGHEST)
        grad_rows = jnp.dot(weights.T, select_cols(out_grads), precision=lax.Precision.HIGHEST)
        return (attended, grad_rows)
    attended, grad_rows = lax.map(per_head, jnp.arange(head_count, dtype=jnp.int32))
    attended = attended.transpose(1, 0, 2).reshape(all_tokens, row_width).astype(jnp.bfloat16)
    value_grads = grad_rows.transpose(1, 0, 2).reshape(all_tokens, row_width).astype(jnp.bfloat16)
    attended_wide = attended.astype(jnp.float32)
    grads_wide = value_grads.astype(jnp.float32)
    input_factor = jnp.dot(attended_wide.T, attended_wide, precision=lax.Precision.HIGHEST) / all_tokens
    grad_factor = jnp.dot(grads_wide.T, grads_wide, precision=lax.Precision.HIGHEST) / all_tokens
    return (input_factor, grad_factor)
```

```python
import math

import jax
import jax.numpy as jnp
from jax import lax
from jax.experimental import pallas as pl
from jax.experimental.pallas import tpu as pltpu
from jax.sharding import PartitionSpec as P

HEAD_DIM = 128


MASK_FLOOR = -1e30


def spread(value, axis, source):
    kept = jnp.where(lax.axis_index(axis) == source, value, 0).astype(value.dtype)
    return lax.psum(kept, axis)


def document_ids(positions, doc_starts):
    return jnp.sum((positions[:, None] >= doc_starts[None, :]).astype(jnp.int32), axis=1) - 1


def pair_scores(query_rows, key_rows, query_pos, key_pos, doc_starts):
    head_count = query_rows.shape[1] // HEAD_DIM
    query_heads = query_rows.reshape(query_rows.shape[0], head_count, HEAD_DIM)
    key_heads = key_rows.reshape(key_rows.shape[0], head_count, HEAD_DIM)
    scores = jnp.einsum(
        "qhd,khd->hqk", query_heads, key_heads, preferred_element_type=jnp.float32
    ) * (1.0 / math.sqrt(HEAD_DIM))
    query_docs = document_ids(query_pos, doc_starts)
    key_docs = document_ids(key_pos, doc_starts)
    allowed = query_docs[:, None] == key_docs[None, :]
    return (scores, allowed[None, :, :])


def on_device(query_in, key_in, value_in, out_grads, doc_starts):
    tok_dev, row_width = query_in.shape
    head_count = row_width // HEAD_DIM
    first_pos = lax.axis_index("tokens") * tok_dev
    query_pos = first_pos + jnp.arange(tok_dev, dtype=jnp.int32)
    keys_all, values_all = (
        lax.all_gather(key_in, "tokens", axis=0, tiled=True),
        lax.all_gather(value_in, "tokens", axis=0, tiled=True),
    )
    all_tokens = keys_all.shape[0]
    key_span = min(512, all_tokens)
    block_ids = jnp.arange(all_tokens // key_span, dtype=jnp.int32)

    def block_scores(block_id):
        key_begin = block_id * key_span
        key_rows = lax.dynamic_slice_in_dim(keys_all, key_begin, key_span, 0)
        key_pos = key_begin + jnp.arange(key_span, dtype=jnp.int32)
        scores, allowed = pair_scores(query_in, key_rows, query_pos, key_pos, doc_starts)
        return (key_begin, scores, allowed)

    def gated(block_id, update, running):
        key_begin = block_id * key_span
        return update(running)

    def stats_step(running, block_id):

        def update(state):
            row_peak, row_mass = state
            key_begin, scores, allowed = block_scores(block_id)
            masked = jnp.where(allowed, scores, MASK_FLOOR)
            new_peak = jnp.maximum(row_peak, jnp.max(masked, axis=2))
            new_mass = row_mass * jnp.exp(row_peak - new_peak) + jnp.sum(
                jnp.where(allowed, jnp.exp(masked - new_peak[:, :, None]), 0.0), axis=2
            )
            return (new_peak, new_mass)

        return (gated(block_id, update, running), None)

    initial = (
        jnp.full((head_count, tok_dev), MASK_FLOOR, jnp.float32),
        jnp.zeros((head_count, tok_dev), jnp.float32),
    )
    (row_peak, row_mass), _ = lax.scan(stats_step, initial, block_ids)
    log_total = row_peak + jnp.log(row_mass)

    def value_step(running, block_id):

        def update(state):
            weighted, partials = state
            key_begin, scores, allowed = block_scores(block_id)
            weights = jnp.where(allowed, jnp.exp(scores - log_total[:, :, None]), 0.0).astype(
                jnp.bfloat16
            )
            value_rows = lax.dynamic_slice_in_dim(values_all, key_begin, key_span, 0).reshape(
                key_span, head_count, HEAD_DIM
            )
            weighted = weighted + jnp.einsum(
                "hqk,khd->qhd", weights, value_rows, preferred_element_type=jnp.float32
            )
            return (weighted, partials)

        return (gated(block_id, update, running), None)

    partial_rows = 8
    value_init = (
        jnp.zeros((tok_dev, head_count, HEAD_DIM), jnp.float32),
        jnp.zeros((partial_rows, row_width), jnp.float32),
    )
    (weighted, partials), _ = lax.scan(value_step, value_init, block_ids)
    attended = weighted.reshape(tok_dev, row_width).astype(jnp.bfloat16)
    stats_all = lax.all_gather(log_total.T, "tokens", axis=0, tiled=True)
    query_rows = lax.all_gather(query_in, "tokens", axis=0, tiled=True)
    grad_rows = lax.all_gather(out_grads, "tokens", axis=0, tiled=True)
    piece_rows = query_rows.shape[0]
    piece_pos = jnp.arange(piece_rows, dtype=jnp.int32)

    def update(grad_sum):
        scores, allowed = pair_scores(query_rows, key_in, piece_pos, query_pos, doc_starts)
        weights = jnp.where(allowed, jnp.exp(scores - stats_all.T[:, :, None]), 0.0).astype(
            jnp.bfloat16
        )
        piece_grads = grad_rows.reshape(piece_rows, head_count, HEAD_DIM)
        return jnp.einsum("hqk,qhd->khd", weights, piece_grads, preferred_element_type=jnp.float32)

    summed = update(jnp.zeros((tok_dev, head_count, HEAD_DIM), jnp.float32))
    value_grads = summed.reshape(tok_dev, row_width).astype(jnp.bfloat16)
    token_shards = lax.axis_size("tokens")
    col_shards = lax.axis_size("cols")
    rows_attended, rows_grads = (
        lax.all_gather(attended[None], ("tokens", "cols"), axis=0, tiled=True),
        lax.all_gather(value_grads[None], ("tokens", "cols"), axis=0, tiled=True),
    )
    rows_attended = rows_attended.reshape(token_shards, col_shards, tok_dev, row_width)
    rows_grads = rows_grads.reshape(token_shards, col_shards, tok_dev, row_width)
    own_attended = lax.dynamic_index_in_dim(
        rows_attended, lax.axis_index("cols"), 1, keepdims=False
    )
    own_grads = lax.dynamic_index_in_dim(rows_grads, lax.axis_index("cols"), 1, keepdims=False)
    cols_attended, cols_grads = (
        spread(own_attended, "heads", lax.axis_index("tokens")),
        spread(own_grads, "heads", lax.axis_index("tokens")),
    )
    input_factor = jnp.einsum(
        "acnf,ang->cfg", rows_attended, cols_attended, preferred_element_type=jnp.float32
    )
    grad_factor = jnp.einsum(
        "acnf,ang->cfg", rows_grads, cols_grads, preferred_element_type=jnp.float32
    )
    input_factor = input_factor.reshape(col_shards * row_width, row_width) / all_tokens
    grad_factor = grad_factor.reshape(col_shards * row_width, row_width) / all_tokens
    return (input_factor, grad_factor)


TO_END = ((1, 1, 0), (1, 1, 1))
QUERY, KEY, VALUE, GRAD = range(4)
MATE, ACROSS, END = range(3)
F32 = jnp.float32
BF16 = jnp.bfloat16


def fused_kernel(
    starts_ref, q_ref, k_ref, v_ref, g_ref, out_a, out_g,
    xin, rows, cols, v_t, g_acc, key_doc, query_doc, stage,
    a2a_send, a2a_recv, row_recv, up_send, down_send, x_send, chunk_send, swap_send,
    col_recv, pair_send, y_send, relay_send, out_sem,
):
    n = lax.axis_size("tokens")
    tok_dev = q_ref.shape[0]
    all_tokens = n * tok_dev
    h = lax.axis_index("heads")
    z = lax.axis_index("tokens")
    x = lax.axis_index("cols")
    y = h // 2
    core = h % 2
    other_x = 1 - x
    pair = y * 2 + (1 - core)
    inputs = (q_ref, k_ref, v_ref, g_ref)
    half = HEAD_DIM // 2
    sources = (z + 1 - 2 * (z % 2), 2 - z // 2, 3 - 3 * (z // 2))

    barrier = pltpu.get_barrier_semaphore()
    for step in range(1, n):
        pl.semaphore_signal(barrier, inc=1, device_id={"tokens": (z + step) % n})
    for step in range(1, 4):
        pl.semaphore_signal(barrier, inc=1, device_id={"heads": (h + step) % 4})
    pl.semaphore_signal(barrier, inc=1, device_id={"cols": other_x})
    pl.semaphore_wait(barrier, n + 3)

    def feature_block(j, a, target):
        return inputs[a].at[:, pl.ds(pl.multiple_of((j * n + target) * HEAD_DIM, HEAD_DIM), HEAD_DIM)]

    def token_block(j, a, source):
        return xin.at[j, a, pl.ds(pl.multiple_of(source * tok_dev, tok_dev), tok_dev), :]

    def own_copy(j, a):
        return pltpu.make_async_copy(
            feature_block(j, a, z), token_block(j, a, z), a2a_recv.at[j, a, z]
        )

    def a2a_copy(j, a, source):
        target = sources[source]
        return pltpu.make_async_remote_copy(
            src_ref=feature_block(j, a, target), dst_ref=token_block(j, a, z),
            send_sem=a2a_send.at[j, a, source], recv_sem=a2a_recv.at[j, a, z],
            device_id={"tokens": target},
        )

    def arrived(j, a, position):
        block = token_block(j, a, position)
        pltpu.make_async_copy(block, block, a2a_recv.at[j, a, position]).wait()

    middle = (z > 0) & (z < n - 1)

    def send_inputs(j, kinds, targets):
        for source in targets:
            for a in kinds:
                a2a_copy(j, a, source).start()

    def send_own(j, kinds):
        for a in kinds:
            own_copy(j, a).start()

    def send_next(kinds):
        @pl.when(jnp.logical_not(middle))
        def _():
            send_inputs(1, kinds, (MATE,))

        for a in kinds:
            for source in (END, ACROSS):
                a2a_copy(1, a, source).start()

    def chunk_copy(position):
        piece = rows.at[0, 0, x, z, :, token_span(position)]
        return pltpu.make_async_remote_copy(
            src_ref=piece, dst_ref=piece, send_sem=chunk_send.at[position],
            recv_sem=row_recv.at[0, 0, x, z, 0], device_id={"cols": other_x},
        )

    def token_span(position):
        return pl.ds(pl.multiple_of(position * tok_dev, tok_dev), tok_dev)

    def attention(j, before, after):
        for position in (z,) + sources:
            arrived(j, VALUE, position)
        v_t[...] = xin[j, VALUE].astype(F32).T.astype(BF16)
        g_acc[...] = jnp.zeros_like(g_acc)

        def step(i, carry):
            position = jnp.where(i == 0, z, jnp.where(i == 1, sources[MATE], jnp.where(i == 2, sources[ACROSS], sources[END])))

            @pl.when(i == 2)
            def _():
                before()

            arrived(j, QUERY, position)
            arrived(j, GRAD, position)

            @pl.when(i == 2)
            def _():
                after()

            attention_block(j, position)
            if j == 0:
                chunk_copy(position).start()
            return carry

        lax.fori_loop(0, n, step, 0)
        rows[j, 1, x, z] = g_acc[...].T.astype(BF16)

    def attention_block(j, position):
        span = token_span(position)
        s = lax.dot_general(
            xin[j, KEY], xin[j, QUERY, span, :], (((1,), (1,)), ((), ())),
            preferred_element_type=F32,
        ) * (1.0 / math.sqrt(HEAD_DIM))
        s = jnp.where(key_doc[...] == query_doc[:, span], s, MASK_FLOOR)
        e = jnp.exp(s - jnp.max(s, axis=0, keepdims=True))
        p = (e * (1.0 / jnp.sum(e, axis=0, keepdims=True))).astype(BF16)
        att = jnp.dot(v_t[...], p, preferred_element_type=F32)
        rows[j, 0, x, z, :, span] = att.astype(BF16)
        g_acc[...] += jnp.dot(p, xin[j, GRAD, span, :], preferred_element_type=F32)

    def row_copy(j, f, xs, zs, part, send, device):
        piece = rows.at[j, f, xs, zs, pl.ds(part * half, half), :]
        return pltpu.make_async_remote_copy(
            src_ref=piece, dst_ref=piece, send_sem=send,
            recv_sem=row_recv.at[j, f, xs, zs, part], device_id=device,
        )

    over_x = {"cols": other_x}
    mate = sources[MATE]

    def up_copy(j, f, part, zs):
        return row_copy(j, f, x, zs, part, up_send.at[j, f, part, zs], {"tokens": (z + 1) % n})

    def down_copy(j, f, part, zs):
        return row_copy(j, f, x, zs, part, down_send.at[j, f, part, zs], {"tokens": (z + n - 1) % n})

    def x_copy(j, f, part, zs):
        return row_copy(j, f, x, zs, part, x_send.at[j, f, part, zs], over_x)

    def swap_copy(j, f, part):
        return row_copy(j, f, other_x, z, part, swap_send.at[j, f, part], {"tokens": mate})

    def own_rows(j, f):
        for part in range(2):
            @pl.when(z < n - 1)
            def _():
                up_copy(j, f, part, z).start()

            @pl.when(z > 0)
            def _():
                down_copy(j, f, part, z).start()

            if (j, f) != (0, 0):
                x_copy(j, f, part, z).start()
        feed_cols(j, f, z)

    def rows_in(j, f, source):
        zs = sources[source]
        for part in range(2):
            x_copy(j, f, part, zs).wait_recv()

            @pl.when((zs < z) & (z < n - 1))
            def _():
                up_copy(j, f, part, zs).start()

            @pl.when((zs > z) & (z > 0))
            def _():
                down_copy(j, f, part, zs).start()

            if source != MATE:
                x_copy(j, f, part, zs).start()
            elif (j, f, part) not in TO_END:
                @pl.when(jnp.logical_not(middle))
                def _():
                    x_copy(j, f, part, zs).start()
        feed_cols(j, f, zs)

    def other_in(j, f, source, part):
        zs = z if source is None else sources[source]
        if (j, f, source) == (0, 0, None):
            if part == 0:
                piece = rows.at[0, 0, other_x, z]
                pltpu.make_async_copy(piece, piece, row_recv.at[0, 0, other_x, z, 0]).wait()
            return
        row_copy(j, f, other_x, zs, part, x_send.at[j, f, part, zs], over_x).wait_recv()

    def swap_rows(j, f, parts):
        for part in parts:
            other_in(j, f, None, part)
        for part in parts:
            swap_copy(j, f, part).start()

    def swap_to_end():
        for j, f, part in TO_END:
            swap_rows(j, f, (part,))

    def other_rows(j, f, group):
        if group == (MATE,):
            for part in range(2):
                if (j, f, part) not in TO_END:
                    @pl.when(middle)
                    def _():
                        other_in(j, f, None, part)
        for source in group:
            for part in range(2):
                other_in(j, f, source, part)

    is_source = h == z
    far = y != z // 2

    def col_copy(j, f, zs, source, send, device):
        return pltpu.make_async_remote_copy(
            src_ref=source, dst_ref=cols.at[j, f, zs], send_sem=send.at[j, f, zs],
            recv_sem=col_recv.at[j, f, zs], device_id={"heads": device},
        )

    def pair_copy(j, f, zs):
        return col_copy(j, f, zs, rows.at[j, f, x, zs], pair_send, pair)

    def y_copy(j, f, zs):
        return col_copy(j, f, zs, rows.at[j, f, x, zs], y_send, (1 - y) * 2 + zs % 2)

    def relay_copy(j, f, zs):
        return col_copy(j, f, zs, cols.at[j, f, zs], relay_send, pair)

    def feed_cols(j, f, zs):
        @pl.when(is_source)
        def _():
            y_copy(j, f, zs).start()
            pair_copy(j, f, zs).start()

    def relay_cols(j, f, source):
        zs = z if source is None else sources[source]

        @pl.when(far & (core == zs % 2))
        def _():
            relay_copy(j, f, zs).wait_recv()
            relay_copy(j, f, zs).start()

    def cols_in(j, f, source):
        zs = z if source is None else sources[source]

        @pl.when(jnp.logical_not(is_source | (far & (core == zs % 2))))
        def _():
            relay_copy(j, f, zs).wait_recv()

        @pl.when(is_source)
        def _():
            cols[j, f, zs] = rows[j, f, x, zs]

    used = [0]
    wide = 2 * HEAD_DIM
    slots = stage.shape[0]

    def out_copy(f, row, col, slot):
        return pltpu.make_async_copy(
            stage.at[slot],
            (out_a, out_g)[f].at[
                pl.ds(pl.multiple_of(row * wide, wide), wide),
                pl.ds(pl.multiple_of(col * wide, wide), wide),
            ],
            out_sem.at[slot],
        )

    def products(f, xs, left, right):
        done = used[0]
        count = len(left) * len(right)

        def one(i, carry):
            at_left, at_right = i // len(right), i % len(right)
            jr = sum(((at_left == k) * item[0] for k, item in enumerate(left)), 0)
            pr = sum(((at_left == k) * item[1] for k, item in enumerate(left)), 0)
            jc = sum(((at_right == k) * item[0] for k, item in enumerate(right)), 0)
            pc = sum(((at_right == k) * item[1] for k, item in enumerate(right)), 0)
            slot = (done + i) % slots

            @pl.when(done + i >= slots)
            def _():
                out_copy(f, 0, 0, slot).wait()

            stage[slot] = (
                lax.dot_general(
                    rows[jr, f, xs, pl.ds(2 * pr, 2)].reshape(wide, all_tokens),
                    cols[jc, f, pl.ds(2 * pc, 2)].reshape(wide, all_tokens),
                    (((1,), (1,)), ((), ())), preferred_element_type=F32,
                ) * (1.0 / all_tokens)
            ).astype(stage.dtype)
            out_copy(f, 4 * xs + 2 * jr + pr, 2 * jc + pc, slot).start()
            return carry

        lax.fori_loop(0, count, one, 0)
        used[0] += count

    for a in (KEY, VALUE):
        send_inputs(0, (a,), (END, ACROSS))
    send_inputs(0, (KEY, VALUE), (MATE,))
    send_own(0, (KEY, VALUE, QUERY, GRAD))
    send_own(1, (KEY, VALUE, QUERY, GRAD))
    doc_count = starts_ref.shape[0]
    key_pos = lax.broadcasted_iota(jnp.int32, key_doc.shape, 0)
    query_pos = lax.broadcasted_iota(jnp.int32, query_doc.shape, 1)
    key_doc[...] = sum((key_pos >= starts_ref[d]).astype(jnp.int32) for d in range(doc_count))
    query_doc[...] = sum((query_pos >= starts_ref[d]).astype(jnp.int32) for d in range(doc_count))
    for position in (z,) + sources:
        arrived(0, KEY, position)
    send_inputs(0, (QUERY, GRAD), (MATE,))
    for a in (QUERY, GRAD):
        send_inputs(0, (a,), (END, ACROSS))

    @pl.when(middle)
    def _():
        send_inputs(1, (KEY, VALUE, QUERY, GRAD), (MATE,))

    def nothing():
        pass

    def send_rest():
        send_next((KEY, VALUE))
        send_next((QUERY, GRAD))

    def at_ends(j, f):
        @pl.when(jnp.logical_not(middle))
        def _():
            rows_in(j, f, MATE)

    def in_middle(j, f):
        @pl.when(middle)
        def _():
            rows_in(j, f, MATE)

    def end_swap(j, f):
        @pl.when(jnp.logical_not(middle))
        def _():
            swap_rows(j, f, range(2))

    attention(0, nothing, send_rest)
    own_rows(0, 0)
    own_rows(0, 1)
    at_ends(0, 0)
    for position in (z,) + sources:
        arrived(1, KEY, position)

    def gather_middle():
        in_middle(0, 0)

    def relay_pair(j, f, group):
        for source in group:
            relay_cols(j, f, source)

    def cols_pair(j, f, group):
        for source in group:
            cols_in(j, f, source)

    attention(1, lambda: at_ends(0, 1), gather_middle)
    near = z // 2
    first, last = (0, near), (0, 1 - near)
    second, final = (1, near), (1, 1 - near)
    own_rows(1, 0)
    own_rows(1, 1)
    in_middle(0, 1)
    at_ends(1, 0)
    end_swap(0, 0)
    end_swap(0, 1)
    at_ends(1, 1)
    rows_in(0, 0, ACROSS)
    in_middle(1, 0)
    end_swap(1, 0)
    rows_in(0, 1, ACROSS)
    in_middle(1, 1)
    end_swap(1, 1)
    relay_pair(0, 0, (None, MATE))
    relay_pair(0, 1, (None, MATE))
    rows_in(0, 0, END)
    relay_pair(1, 0, (None, MATE))
    relay_pair(1, 1, (None,))
    cols_pair(0, 0, (None, MATE))
    cols_pair(1, 0, (None, MATE))
    products(0, x, (first, second), (first, second))
    rows_in(0, 1, END)
    relay_pair(0, 0, (ACROSS,))
    relay_pair(0, 1, (ACROSS,))
    relay_pair(1, 1, (MATE,))
    cols_pair(0, 1, (None, MATE))
    cols_pair(1, 1, (None, MATE))
    products(1, x, (first, second), (first, second))
    rows_in(1, 0, ACROSS)
    relay_pair(0, 0, (END,))
    cols_pair(0, 0, (ACROSS, END))
    products(0, x, (last,), (first, second, last))
    products(0, x, (first, second), (last,))
    rows_in(1, 1, ACROSS)
    relay_pair(0, 1, (END,))
    relay_pair(1, 0, (ACROSS,))
    cols_pair(0, 1, (ACROSS, END))
    products(1, x, (last,), (first, second, last))
    products(1, x, (first, second), (last,))
    other_rows(0, 0, (MATE,))
    other_rows(1, 0, (MATE,))
    products(0, other_x, (first, second), (first, second, last))
    rows_in(1, 0, END)
    relay_pair(1, 1, (ACROSS,))
    other_rows(0, 1, (MATE,))
    products(1, other_x, (first,), (first, second, last))
    other_rows(0, 0, (ACROSS, END))
    products(0, other_x, (last,), (first, second, last))
    relay_pair(1, 0, (END,))
    cols_pair(1, 0, (ACROSS, END))
    products(0, x, (final,), (first, second, last, final))
    products(0, x, (first, second, last), (final,))
    rows_in(1, 1, END)

    @pl.when(middle)
    def _():
        swap_to_end()

    products(0, other_x, (first, second, last), (final,))
    other_rows(0, 1, (ACROSS, END))
    products(1, other_x, (last,), (first, second, last))
    products(1, x, (final,), (first, second, last))
    relay_pair(1, 1, (END,))
    other_rows(1, 0, (ACROSS, END))
    products(0, other_x, (final,), (first, second, last, final))
    cols_pair(1, 1, (ACROSS, END))
    products(1, x, (first, second, last, final), (final,))
    products(1, other_x, (first, last), (final,))
    other_rows(1, 1, (MATE,))
    products(1, other_x, (second,), (first, second, last, final))
    other_rows(1, 1, (ACROSS, END))
    products(1, other_x, (final,), (first, second, last, final))
    for slot in range(slots):
        out_copy(0, 0, 0, slot).wait()

    for j in range(2):
        for a in range(4):
            for source in range(3):
                a2a_copy(j, a, source).wait_send()
        for f in range(2):
            for part in range(2):
                def sent(zs, carry):
                    own_chunks = (zs == z) if (j, f) == (0, 0) else False
                    swapped = (zs == mate) if (j, f, part) in TO_END else (zs == mate) & middle

                    @pl.when(jnp.logical_not(swapped | own_chunks))
                    def _():
                        x_copy(j, f, part, zs).wait_send()

                    if (j, f, part) == (0, 0, 0):
                        chunk_copy(zs).wait_send()

                    @pl.when((z < n - 1) & (zs <= z))
                    def _():
                        up_copy(j, f, part, zs).wait_send()

                    @pl.when((z > 0) & (zs >= z))
                    def _():
                        down_copy(j, f, part, zs).wait_send()

                    return carry

                lax.fori_loop(0, n, sent, 0)
            for zs in range(n):
                @pl.when(is_source)
                def _():
                    pair_copy(j, f, zs).wait_send()
                    y_copy(j, f, zs).wait_send()

                @pl.when(far & (core == zs % 2))
                def _():
                    relay_copy(j, f, zs).wait_send()
    for j in range(2):
        for f in range(2):
            for part in range(2):
                if (j, f, part) in TO_END:
                    swap_copy(j, f, part).wait_send()
                else:
                    @pl.when(jnp.logical_not(middle))
                    def _():
                        swap_copy(j, f, part).wait_send()


def fused(query_in, key_in, value_in, out_grads, doc_starts):
    n = lax.axis_size("tokens")
    tok_dev, row_width = query_in.shape
    all_tokens = n * tok_dev
    dma = pltpu.SemaphoreType.DMA
    hbm = pl.BlockSpec(memory_space=pl.ANY)
    smem = pl.BlockSpec(memory_space=pltpu.SMEM)
    out = jax.ShapeDtypeStruct((2 * row_width, row_width), F32)
    return tuple(pl.pallas_call(
        fused_kernel,
        out_shape=(out, out),
        in_specs=[smem] + [hbm] * 4,
        out_specs=[hbm] * 2,
        scratch_shapes=[
            pltpu.VMEM((2, 4, all_tokens, HEAD_DIM), BF16),
            pltpu.VMEM((2, 2, 2, n, HEAD_DIM, all_tokens), BF16),
            pltpu.VMEM((2, 2, n, HEAD_DIM, all_tokens), BF16),
            pltpu.VMEM((HEAD_DIM, all_tokens), BF16),
            pltpu.VMEM((all_tokens, HEAD_DIM), F32),
            pltpu.VMEM((all_tokens, 1), jnp.int32),
            pltpu.VMEM((1, all_tokens), jnp.int32),
            pltpu.VMEM((8, 2 * HEAD_DIM, 2 * HEAD_DIM), F32),
            dma((2, 4, 3)), dma((2, 4, n)), dma((2, 2, 2, n, 2)),
            dma((2, 2, 2, n)), dma((2, 2, 2, n)), dma((2, 2, 2, n)), dma((n,)), dma((2, 2, 2)),
            dma((2, 2, n)), dma((2, 2, n)), dma((2, 2, n)), dma((2, 2, n)), dma((8,)),
        ],
        compiler_params=pltpu.CompilerParams(
            collective_id=0, has_side_effects=True, vmem_limit_bytes=60 * 1024 * 1024
        ),
    )(doc_starts, query_in, key_in, value_in, out_grads))


def per_device(query_in, key_in, value_in, out_grads, doc_starts):
    n = lax.axis_size("tokens")
    fits = n == 4 and lax.axis_size("heads") == 4 and lax.axis_size("cols") == 2
    if fits and query_in.shape[1] == 2 * n * HEAD_DIM and query_in.shape[0] % HEAD_DIM == 0:
        return fused(query_in, key_in, value_in, out_grads, doc_starts)
    return on_device(query_in, key_in, value_in, out_grads, doc_starts)


def solution(mesh):
    in_specs = (
        P("tokens", ("heads", "cols")),
        P("tokens", ("heads", "cols")),
        P("tokens", ("heads", "cols")),
        P("tokens", ("heads", "cols")),
        P(),
    )
    out_specs = (P("heads", ("tokens", "cols")), P("heads", ("tokens", "cols")))
    return jax.shard_map(
        per_device, mesh=mesh, in_specs=in_specs, out_specs=out_specs, check_vma=False
    )
```

```python
import math

import jax
import jax.numpy as jnp
from jax import lax
from jax.experimental import pallas as pl
from jax.experimental.pallas import tpu as pltpu
from jax.sharding import PartitionSpec as P

HEAD_DIM = 128


MASK_FLOOR = -1e30


def spread(value, axis, source):
    kept = jnp.where(lax.axis_index(axis) == source, value, 0).astype(value.dtype)
    return lax.psum(kept, axis)


def document_ids(positions, doc_starts):
    return jnp.sum((positions[:, None] >= doc_starts[None, :]).astype(jnp.int32), axis=1) - 1


def pair_scores(query_rows, key_rows, query_pos, key_pos, doc_starts):
    head_count = query_rows.shape[1] // HEAD_DIM
    query_heads = query_rows.reshape(query_rows.shape[0], head_count, HEAD_DIM)
    key_heads = key_rows.reshape(key_rows.shape[0], head_count, HEAD_DIM)
    scores = jnp.einsum(
        "qhd,khd->hqk", query_heads, key_heads, preferred_element_type=jnp.float32
    ) * (1.0 / math.sqrt(HEAD_DIM))
    query_docs = document_ids(query_pos, doc_starts)
    key_docs = document_ids(key_pos, doc_starts)
    allowed = query_docs[:, None] == key_docs[None, :]
    return (scores, allowed[None, :, :])


def on_device(query_in, key_in, value_in, out_grads, doc_starts):
    tok_dev, row_width = query_in.shape
    head_count = row_width // HEAD_DIM
    first_pos = lax.axis_index("tokens") * tok_dev
    query_pos = first_pos + jnp.arange(tok_dev, dtype=jnp.int32)
    keys_all, values_all = (
        lax.all_gather(key_in, "tokens", axis=0, tiled=True),
        lax.all_gather(value_in, "tokens", axis=0, tiled=True),
    )
    all_tokens = keys_all.shape[0]
    key_span = min(512, all_tokens)
    block_ids = jnp.arange(all_tokens // key_span, dtype=jnp.int32)

    def block_scores(block_id):
        key_begin = block_id * key_span
        key_rows = lax.dynamic_slice_in_dim(keys_all, key_begin, key_span, 0)
        key_pos = key_begin + jnp.arange(key_span, dtype=jnp.int32)
        scores, allowed = pair_scores(query_in, key_rows, query_pos, key_pos, doc_starts)
        return (key_begin, scores, allowed)

    def gated(block_id, update, running):
        key_begin = block_id * key_span
        return update(running)

    def stats_step(running, block_id):

        def update(state):
            row_peak, row_mass = state
            key_begin, scores, allowed = block_scores(block_id)
            masked = jnp.where(allowed, scores, MASK_FLOOR)
            new_peak = jnp.maximum(row_peak, jnp.max(masked, axis=2))
            new_mass = row_mass * jnp.exp(row_peak - new_peak) + jnp.sum(
                jnp.where(allowed, jnp.exp(masked - new_peak[:, :, None]), 0.0), axis=2
            )
            return (new_peak, new_mass)

        return (gated(block_id, update, running), None)

    initial = (
        jnp.full((head_count, tok_dev), MASK_FLOOR, jnp.float32),
        jnp.zeros((head_count, tok_dev), jnp.float32),
    )
    (row_peak, row_mass), _ = lax.scan(stats_step, initial, block_ids)
    log_total = row_peak + jnp.log(row_mass)

    def value_step(running, block_id):

        def update(state):
            weighted, partials = state
            key_begin, scores, allowed = block_scores(block_id)
            weights = jnp.where(allowed, jnp.exp(scores - log_total[:, :, None]), 0.0).astype(
                jnp.bfloat16
            )
            value_rows = lax.dynamic_slice_in_dim(values_all, key_begin, key_span, 0).reshape(
                key_span, head_count, HEAD_DIM
            )
            weighted = weighted + jnp.einsum(
                "hqk,khd->qhd", weights, value_rows, preferred_element_type=jnp.float32
            )
            return (weighted, partials)

        return (gated(block_id, update, running), None)

    partial_rows = 8
    value_init = (
        jnp.zeros((tok_dev, head_count, HEAD_DIM), jnp.float32),
        jnp.zeros((partial_rows, row_width), jnp.float32),
    )
    (weighted, partials), _ = lax.scan(value_step, value_init, block_ids)
    attended = weighted.reshape(tok_dev, row_width).astype(jnp.bfloat16)
    stats_all = lax.all_gather(log_total.T, "tokens", axis=0, tiled=True)
    query_rows = lax.all_gather(query_in, "tokens", axis=0, tiled=True)
    grad_rows = lax.all_gather(out_grads, "tokens", axis=0, tiled=True)
    piece_rows = query_rows.shape[0]
    piece_pos = jnp.arange(piece_rows, dtype=jnp.int32)

    def update(grad_sum):
        scores, allowed = pair_scores(query_rows, key_in, piece_pos, query_pos, doc_starts)
        weights = jnp.where(allowed, jnp.exp(scores - stats_all.T[:, :, None]), 0.0).astype(
            jnp.bfloat16
        )
        piece_grads = grad_rows.reshape(piece_rows, head_count, HEAD_DIM)
        return jnp.einsum("hqk,qhd->khd", weights, piece_grads, preferred_element_type=jnp.float32)

    summed = update(jnp.zeros((tok_dev, head_count, HEAD_DIM), jnp.float32))
    value_grads = summed.reshape(tok_dev, row_width).astype(jnp.bfloat16)
    token_shards = lax.axis_size("tokens")
    col_shards = lax.axis_size("cols")
    rows_attended, rows_grads = (
        lax.all_gather(attended[None], ("tokens", "cols"), axis=0, tiled=True),
        lax.all_gather(value_grads[None], ("tokens", "cols"), axis=0, tiled=True),
    )
    rows_attended = rows_attended.reshape(token_shards, col_shards, tok_dev, row_width)
    rows_grads = rows_grads.reshape(token_shards, col_shards, tok_dev, row_width)
    own_attended = lax.dynamic_index_in_dim(
        rows_attended, lax.axis_index("cols"), 1, keepdims=False
    )
    own_grads = lax.dynamic_index_in_dim(rows_grads, lax.axis_index("cols"), 1, keepdims=False)
    cols_attended, cols_grads = (
        spread(own_attended, "heads", lax.axis_index("tokens")),
        spread(own_grads, "heads", lax.axis_index("tokens")),
    )
    input_factor = jnp.einsum(
        "acnf,ang->cfg", rows_attended, cols_attended, preferred_element_type=jnp.float32
    )
    grad_factor = jnp.einsum(
        "acnf,ang->cfg", rows_grads, cols_grads, preferred_element_type=jnp.float32
    )
    input_factor = input_factor.reshape(col_shards * row_width, row_width) / all_tokens
    grad_factor = grad_factor.reshape(col_shards * row_width, row_width) / all_tokens
    return (input_factor, grad_factor)


TO_END = ((1, 1, 0), (1, 1, 1))
QUERY, KEY, VALUE, GRAD = range(4)
MATE, ACROSS, END = range(3)
F32 = jnp.float32
BF16 = jnp.bfloat16


def fused_kernel(
    starts_ref, q_ref, k_ref, v_ref, g_ref, out_a, out_g,
    xin, rows, cols, v_t, g_acc, key_doc, query_doc,
    a2a_send, a2a_recv, row_recv, up_send, down_send, x_send, chunk_send, swap_send,
    col_recv, pair_send, y_send, relay_send,
):
    n = lax.axis_size("tokens")
    tok_dev = q_ref.shape[0]
    all_tokens = n * tok_dev
    h = lax.axis_index("heads")
    z = lax.axis_index("tokens")
    x = lax.axis_index("cols")
    y = h // 2
    core = h % 2
    other_x = 1 - x
    pair = y * 2 + (1 - core)
    inputs = (q_ref, k_ref, v_ref, g_ref)
    half = HEAD_DIM // 2
    sources = (z + 1 - 2 * (z % 2), 2 - z // 2, 3 - 3 * (z // 2))

    barrier = pltpu.get_barrier_semaphore()
    for step in range(1, n):
        pl.semaphore_signal(barrier, inc=1, device_id={"tokens": (z + step) % n})
    for step in range(1, 4):
        pl.semaphore_signal(barrier, inc=1, device_id={"heads": (h + step) % 4})
    pl.semaphore_signal(barrier, inc=1, device_id={"cols": other_x})
    pl.semaphore_wait(barrier, n + 3)

    def feature_block(j, a, target):
        return inputs[a].at[:, pl.ds(pl.multiple_of((j * n + target) * HEAD_DIM, HEAD_DIM), HEAD_DIM)]

    def token_block(j, a, source):
        return xin.at[j, a, pl.ds(pl.multiple_of(source * tok_dev, tok_dev), tok_dev), :]

    def own_copy(j, a):
        return pltpu.make_async_copy(
            feature_block(j, a, z), token_block(j, a, z), a2a_recv.at[j, a, z]
        )

    def a2a_copy(j, a, source):
        target = sources[source]
        return pltpu.make_async_remote_copy(
            src_ref=feature_block(j, a, target), dst_ref=token_block(j, a, z),
            send_sem=a2a_send.at[j, a, source], recv_sem=a2a_recv.at[j, a, z],
            device_id={"tokens": target},
        )

    def arrived(j, a, position):
        block = token_block(j, a, position)
        pltpu.make_async_copy(block, block, a2a_recv.at[j, a, position]).wait()

    middle = (z > 0) & (z < n - 1)

    def send_inputs(j, kinds, targets):
        for source in targets:
            for a in kinds:
                a2a_copy(j, a, source).start()

    def send_own(j, kinds):
        for a in kinds:
            own_copy(j, a).start()

    def send_next(kinds):
        @pl.when(jnp.logical_not(middle))
        def _():
            send_inputs(1, kinds, (MATE,))

        for a in kinds:
            for source in (END, ACROSS):
                a2a_copy(1, a, source).start()

    def chunk_copy(position):
        piece = rows.at[0, 0, x, z, :, token_span(position)]
        return pltpu.make_async_remote_copy(
            src_ref=piece, dst_ref=piece, send_sem=chunk_send.at[position],
            recv_sem=row_recv.at[0, 0, x, z, 0], device_id={"cols": other_x},
        )

    def token_span(position):
        return pl.ds(pl.multiple_of(position * tok_dev, tok_dev), tok_dev)

    def attention(j, before, after):
        for position in (z,) + sources:
            arrived(j, VALUE, position)
        v_t[...] = xin[j, VALUE].astype(F32).T.astype(BF16)
        g_acc[...] = jnp.zeros_like(g_acc)

        def step(i, carry):
            position = jnp.where(i == 0, z, jnp.where(i == 1, sources[MATE], jnp.where(i == 2, sources[ACROSS], sources[END])))

            @pl.when(i == 2)
            def _():
                before()

            arrived(j, QUERY, position)
            arrived(j, GRAD, position)

            @pl.when(i == 2)
            def _():
                after()

            attention_block(j, position)
            if j == 0:
                chunk_copy(position).start()
            return carry

        lax.fori_loop(0, n, step, 0)
        rows[j, 1, x, z] = g_acc[...].T.astype(BF16)

    def attention_block(j, position):
        span = token_span(position)
        s = lax.dot_general(
            xin[j, KEY], xin[j, QUERY, span, :], (((1,), (1,)), ((), ())),
            preferred_element_type=F32,
        ) * (1.0 / math.sqrt(HEAD_DIM))
        s = jnp.where(key_doc[...] == query_doc[:, span], s, MASK_FLOOR)
        e = jnp.exp(s - jnp.max(s, axis=0, keepdims=True))
        p = (e * (1.0 / jnp.sum(e, axis=0, keepdims=True))).astype(BF16)
        att = jnp.dot(v_t[...], p, preferred_element_type=F32)
        rows[j, 0, x, z, :, span] = att.astype(BF16)
        g_acc[...] += jnp.dot(p, xin[j, GRAD, span, :], preferred_element_type=F32)

    def row_copy(j, f, xs, zs, part, send, device):
        piece = rows.at[j, f, xs, zs, pl.ds(part * half, half), :]
        return pltpu.make_async_remote_copy(
            src_ref=piece, dst_ref=piece, send_sem=send,
            recv_sem=row_recv.at[j, f, xs, zs, part], device_id=device,
        )

    over_x = {"cols": other_x}
    mate = sources[MATE]

    def up_copy(j, f, part, zs):
        return row_copy(j, f, x, zs, part, up_send.at[j, f, part, zs], {"tokens": (z + 1) % n})

    def down_copy(j, f, part, zs):
        return row_copy(j, f, x, zs, part, down_send.at[j, f, part, zs], {"tokens": (z + n - 1) % n})

    def x_copy(j, f, part, zs):
        return row_copy(j, f, x, zs, part, x_send.at[j, f, part, zs], over_x)

    def swap_copy(j, f, part):
        return row_copy(j, f, other_x, z, part, swap_send.at[j, f, part], {"tokens": mate})

    def own_rows(j, f):
        for part in range(2):
            @pl.when(z < n - 1)
            def _():
                up_copy(j, f, part, z).start()

            @pl.when(z > 0)
            def _():
                down_copy(j, f, part, z).start()

            if (j, f) != (0, 0):
                x_copy(j, f, part, z).start()
        feed_cols(j, f, z)

    def rows_in(j, f, source):
        zs = sources[source]
        for part in range(2):
            x_copy(j, f, part, zs).wait_recv()

            @pl.when((zs < z) & (z < n - 1))
            def _():
                up_copy(j, f, part, zs).start()

            @pl.when((zs > z) & (z > 0))
            def _():
                down_copy(j, f, part, zs).start()

            if source != MATE:
                x_copy(j, f, part, zs).start()
            elif (j, f, part) not in TO_END:
                @pl.when(jnp.logical_not(middle))
                def _():
                    x_copy(j, f, part, zs).start()
        feed_cols(j, f, zs)

    def other_in(j, f, source, part):
        zs = z if source is None else sources[source]
        if (j, f, source) == (0, 0, None):
            if part == 0:
                piece = rows.at[0, 0, other_x, z]
                pltpu.make_async_copy(piece, piece, row_recv.at[0, 0, other_x, z, 0]).wait()
            return
        row_copy(j, f, other_x, zs, part, x_send.at[j, f, part, zs], over_x).wait_recv()

    def swap_rows(j, f, parts):
        for part in parts:
            other_in(j, f, None, part)
        for part in parts:
            swap_copy(j, f, part).start()

    def swap_to_end():
        for j, f, part in TO_END:
            swap_rows(j, f, (part,))

    def other_rows(j, f, group):
        if group == (MATE,):
            for part in range(2):
                if (j, f, part) not in TO_END:
                    @pl.when(middle)
                    def _():
                        other_in(j, f, None, part)
        for source in group:
            for part in range(2):
                other_in(j, f, source, part)

    is_source = h == z
    far = y != z // 2

    def col_copy(j, f, zs, source, send, device):
        return pltpu.make_async_remote_copy(
            src_ref=source, dst_ref=cols.at[j, f, zs], send_sem=send.at[j, f, zs],
            recv_sem=col_recv.at[j, f, zs], device_id={"heads": device},
        )

    def pair_copy(j, f, zs):
        return col_copy(j, f, zs, rows.at[j, f, x, zs], pair_send, pair)

    def y_copy(j, f, zs):
        return col_copy(j, f, zs, rows.at[j, f, x, zs], y_send, (1 - y) * 2 + zs % 2)

    def relay_copy(j, f, zs):
        return col_copy(j, f, zs, cols.at[j, f, zs], relay_send, pair)

    def feed_cols(j, f, zs):
        @pl.when(is_source)
        def _():
            y_copy(j, f, zs).start()
            pair_copy(j, f, zs).start()

    def relay_cols(j, f, source):
        zs = z if source is None else sources[source]

        @pl.when(far & (core == zs % 2))
        def _():
            relay_copy(j, f, zs).wait_recv()
            relay_copy(j, f, zs).start()

    def cols_in(j, f, source):
        zs = z if source is None else sources[source]

        @pl.when(jnp.logical_not(is_source | (far & (core == zs % 2))))
        def _():
            relay_copy(j, f, zs).wait_recv()

        @pl.when(is_source)
        def _():
            cols[j, f, zs] = rows[j, f, x, zs]

    wide = 2 * HEAD_DIM

    def products(f, xs, left, right):
        count = len(left) * len(right)

        def one(i, carry):
            at_left, at_right = i // len(right), i % len(right)
            jr = sum(((at_left == k) * item[0] for k, item in enumerate(left)), 0)
            pr = sum(((at_left == k) * item[1] for k, item in enumerate(left)), 0)
            jc = sum(((at_right == k) * item[0] for k, item in enumerate(right)), 0)
            pc = sum(((at_right == k) * item[1] for k, item in enumerate(right)), 0)
            row = pl.multiple_of((4 * xs + 2 * jr + pr) * wide, wide)
            col = pl.multiple_of((2 * jc + pc) * wide, wide)
            (out_a, out_g)[f][pl.ds(row, wide), pl.ds(col, wide)] = lax.dot_general(
                rows[jr, f, xs, pl.ds(2 * pr, 2)].reshape(wide, all_tokens),
                cols[jc, f, pl.ds(2 * pc, 2)].reshape(wide, all_tokens),
                (((1,), (1,)), ((), ())), preferred_element_type=F32,
            ) * (1.0 / all_tokens)
            return carry

        lax.fori_loop(0, count, one, 0)

    for a in (KEY, VALUE):
        send_inputs(0, (a,), (END, ACROSS))
    send_inputs(0, (KEY, VALUE), (MATE,))
    send_own(0, (KEY, VALUE, QUERY, GRAD))
    send_own(1, (KEY, VALUE, QUERY, GRAD))
    doc_count = starts_ref.shape[0]
    key_pos = lax.broadcasted_iota(jnp.int32, key_doc.shape, 0)
    query_pos = lax.broadcasted_iota(jnp.int32, query_doc.shape, 1)
    key_doc[...] = sum((key_pos >= starts_ref[d]).astype(jnp.int32) for d in range(doc_count))
    query_doc[...] = sum((query_pos >= starts_ref[d]).astype(jnp.int32) for d in range(doc_count))
    for position in (z,) + sources:
        arrived(0, KEY, position)
    send_inputs(0, (QUERY, GRAD), (MATE,))
    for a in (QUERY, GRAD):
        send_inputs(0, (a,), (END, ACROSS))

    @pl.when(middle)
    def _():
        send_inputs(1, (KEY, VALUE, QUERY, GRAD), (MATE,))

    def nothing():
        pass

    def send_rest():
        send_next((KEY, VALUE))
        send_next((QUERY, GRAD))

    def at_ends(j, f):
        @pl.when(jnp.logical_not(middle))
        def _():
            rows_in(j, f, MATE)

    def in_middle(j, f):
        @pl.when(middle)
        def _():
            rows_in(j, f, MATE)

    def end_swap(j, f):
        @pl.when(jnp.logical_not(middle))
        def _():
            swap_rows(j, f, range(2))

    attention(0, nothing, send_rest)
    own_rows(0, 0)
    own_rows(0, 1)
    at_ends(0, 0)
    for position in (z,) + sources:
        arrived(1, KEY, position)

    def gather_middle():
        in_middle(0, 0)

    def relay_pair(j, f, group):
        for source in group:
            relay_cols(j, f, source)

    def cols_pair(j, f, group):
        for source in group:
            cols_in(j, f, source)

    attention(1, lambda: at_ends(0, 1), gather_middle)
    near = z // 2
    first, last = (0, near), (0, 1 - near)
    second, final = (1, near), (1, 1 - near)
    own_rows(1, 0)
    own_rows(1, 1)
    in_middle(0, 1)
    at_ends(1, 0)
    end_swap(0, 0)
    end_swap(0, 1)
    at_ends(1, 1)
    rows_in(0, 0, ACROSS)
    in_middle(1, 0)
    end_swap(1, 0)
    rows_in(0, 1, ACROSS)
    in_middle(1, 1)
    end_swap(1, 1)
    relay_pair(0, 0, (None, MATE))
    relay_pair(0, 1, (None, MATE))
    rows_in(0, 0, END)
    relay_pair(1, 0, (None, MATE))
    relay_pair(1, 1, (None,))
    cols_pair(0, 0, (None, MATE))
    cols_pair(1, 0, (None, MATE))
    products(0, x, (first, second), (first, second))
    rows_in(0, 1, END)
    relay_pair(0, 0, (ACROSS,))
    relay_pair(0, 1, (ACROSS,))
    relay_pair(1, 1, (MATE,))
    cols_pair(0, 1, (None, MATE))
    cols_pair(1, 1, (None, MATE))
    products(1, x, (first, second), (first, second))
    rows_in(1, 0, ACROSS)
    relay_pair(0, 0, (END,))
    cols_pair(0, 0, (ACROSS, END))
    products(0, x, (last,), (first, second, last))
    products(0, x, (first, second), (last,))
    rows_in(1, 1, ACROSS)
    relay_pair(0, 1, (END,))
    relay_pair(1, 0, (ACROSS,))
    cols_pair(0, 1, (ACROSS, END))
    products(1, x, (last,), (first, second, last))
    products(1, x, (first, second), (last,))
    other_rows(0, 0, (MATE,))
    other_rows(1, 0, (MATE,))
    products(0, other_x, (first, second), (first, second, last))
    rows_in(1, 0, END)
    relay_pair(1, 1, (ACROSS,))
    other_rows(0, 1, (MATE,))
    products(1, other_x, (first,), (first, second, last))
    other_rows(0, 0, (ACROSS, END))
    products(0, other_x, (last,), (first, second, last))
    relay_pair(1, 0, (END,))
    cols_pair(1, 0, (ACROSS, END))
    products(0, x, (final,), (first, second, last, final))
    products(0, x, (first, second, last), (final,))
    rows_in(1, 1, END)

    @pl.when(middle)
    def _():
        swap_to_end()

    products(0, other_x, (first, second, last), (final,))
    other_rows(0, 1, (ACROSS, END))
    products(1, other_x, (last,), (first, second, last))
    products(1, x, (final,), (first, second, last))
    relay_pair(1, 1, (END,))
    other_rows(1, 0, (ACROSS, END))
    products(0, other_x, (final,), (first, second, last, final))
    cols_pair(1, 1, (ACROSS, END))
    products(1, x, (first, second, last, final), (final,))
    products(1, other_x, (first, last), (final,))
    other_rows(1, 1, (MATE,))
    products(1, other_x, (second,), (first, second, last, final))
    other_rows(1, 1, (ACROSS, END))
    products(1, other_x, (final,), (first, second, last, final))
    for j in range(2):
        for a in range(4):
            for source in range(3):
                a2a_copy(j, a, source).wait_send()
        for f in range(2):
            for part in range(2):
                def sent(zs, carry):
                    own_chunks = (zs == z) if (j, f) == (0, 0) else False
                    swapped = (zs == mate) if (j, f, part) in TO_END else (zs == mate) & middle

                    @pl.when(jnp.logical_not(swapped | own_chunks))
                    def _():
                        x_copy(j, f, part, zs).wait_send()

                    if (j, f, part) == (0, 0, 0):
                        chunk_copy(zs).wait_send()

                    @pl.when((z < n - 1) & (zs <= z))
                    def _():
                        up_copy(j, f, part, zs).wait_send()

                    @pl.when((z > 0) & (zs >= z))
                    def _():
                        down_copy(j, f, part, zs).wait_send()

                    return carry

                lax.fori_loop(0, n, sent, 0)
            for zs in range(n):
                @pl.when(is_source)
                def _():
                    pair_copy(j, f, zs).wait_send()
                    y_copy(j, f, zs).wait_send()

                @pl.when(far & (core == zs % 2))
                def _():
                    relay_copy(j, f, zs).wait_send()
    for j in range(2):
        for f in range(2):
            for part in range(2):
                if (j, f, part) in TO_END:
                    swap_copy(j, f, part).wait_send()
                else:
                    @pl.when(jnp.logical_not(middle))
                    def _():
                        swap_copy(j, f, part).wait_send()


def fused(query_in, key_in, value_in, out_grads, doc_starts):
    n = lax.axis_size("tokens")
    tok_dev, row_width = query_in.shape
    all_tokens = n * tok_dev
    dma = pltpu.SemaphoreType.DMA
    hbm = pl.BlockSpec(memory_space=pl.ANY)
    smem = pl.BlockSpec(memory_space=pltpu.SMEM)
    out = pltpu.VMEM((2 * row_width, row_width), F32)
    return tuple(pl.pallas_call(
        fused_kernel,
        out_shape=(out, out),
        in_specs=[smem] + [hbm] * 4,
        out_specs=[pl.BlockSpec(memory_space=pltpu.VMEM)] * 2,
        scratch_shapes=[
            pltpu.VMEM((2, 4, all_tokens, HEAD_DIM), BF16),
            pltpu.VMEM((2, 2, 2, n, HEAD_DIM, all_tokens), BF16),
            pltpu.VMEM((2, 2, n, HEAD_DIM, all_tokens), BF16),
            pltpu.VMEM((HEAD_DIM, all_tokens), BF16),
            pltpu.VMEM((all_tokens, HEAD_DIM), F32),
            pltpu.VMEM((all_tokens, 1), jnp.int32),
            pltpu.VMEM((1, all_tokens), jnp.int32),
            dma((2, 4, 3)), dma((2, 4, n)), dma((2, 2, 2, n, 2)),
            dma((2, 2, 2, n)), dma((2, 2, 2, n)), dma((2, 2, 2, n)), dma((n,)), dma((2, 2, 2)),
            dma((2, 2, n)), dma((2, 2, n)), dma((2, 2, n)), dma((2, 2, n)),
        ],
        compiler_params=pltpu.CompilerParams(
            collective_id=0, has_side_effects=True, vmem_limit_bytes=38 * 1024 * 1024
        ),
    )(doc_starts, query_in, key_in, value_in, out_grads))


def per_device(query_in, key_in, value_in, out_grads, doc_starts):
    n = lax.axis_size("tokens")
    fits = n == 4 and lax.axis_size("heads") == 4 and lax.axis_size("cols") == 2
    if fits and query_in.shape[1] == 2 * n * HEAD_DIM and query_in.shape[0] % HEAD_DIM == 0:
        return fused(query_in, key_in, value_in, out_grads, doc_starts)
    return on_device(query_in, key_in, value_in, out_grads, doc_starts)


def solution(mesh):
    in_specs = (
        P("tokens", ("heads", "cols")),
        P("tokens", ("heads", "cols")),
        P("tokens", ("heads", "cols")),
        P("tokens", ("heads", "cols")),
        P(),
    )
    out_specs = (P("heads", ("tokens", "cols")), P("heads", ("tokens", "cols")))
    return jax.shard_map(
        per_device, mesh=mesh, in_specs=in_specs, out_specs=out_specs, check_vma=False
    )
```

```python
import math

import jax
import jax.numpy as jnp
from jax import lax
from jax.experimental import pallas as pl
from jax.experimental.pallas import tpu as pltpu
from jax.sharding import PartitionSpec as P

HEAD_DIM = 128


MASK_FLOOR = -1e30


def spread(value, axis, source):
    kept = jnp.where(lax.axis_index(axis) == source, value, 0).astype(value.dtype)
    return lax.psum(kept, axis)


def document_ids(positions, doc_starts):
    return jnp.sum((positions[:, None] >= doc_starts[None, :]).astype(jnp.int32), axis=1) - 1


def pair_scores(query_rows, key_rows, query_pos, key_pos, doc_starts):
    head_count = query_rows.shape[1] // HEAD_DIM
    query_heads = query_rows.reshape(query_rows.shape[0], head_count, HEAD_DIM)
    key_heads = key_rows.reshape(key_rows.shape[0], head_count, HEAD_DIM)
    scores = jnp.einsum(
        "qhd,khd->hqk", query_heads, key_heads, preferred_element_type=jnp.float32
    ) * (1.0 / math.sqrt(HEAD_DIM))
    query_docs = document_ids(query_pos, doc_starts)
    key_docs = document_ids(key_pos, doc_starts)
    allowed = query_docs[:, None] == key_docs[None, :]
    return (scores, allowed[None, :, :])


def on_device(query_in, key_in, value_in, out_grads, doc_starts):
    tok_dev, row_width = query_in.shape
    head_count = row_width // HEAD_DIM
    first_pos = lax.axis_index("tokens") * tok_dev
    query_pos = first_pos + jnp.arange(tok_dev, dtype=jnp.int32)
    keys_all, values_all = (
        lax.all_gather(key_in, "tokens", axis=0, tiled=True),
        lax.all_gather(value_in, "tokens", axis=0, tiled=True),
    )
    all_tokens = keys_all.shape[0]
    key_span = min(512, all_tokens)
    block_ids = jnp.arange(all_tokens // key_span, dtype=jnp.int32)

    def block_scores(block_id):
        key_begin = block_id * key_span
        key_rows = lax.dynamic_slice_in_dim(keys_all, key_begin, key_span, 0)
        key_pos = key_begin + jnp.arange(key_span, dtype=jnp.int32)
        scores, allowed = pair_scores(query_in, key_rows, query_pos, key_pos, doc_starts)
        return (key_begin, scores, allowed)

    def gated(block_id, update, running):
        key_begin = block_id * key_span
        return update(running)

    def stats_step(running, block_id):

        def update(state):
            row_peak, row_mass = state
            key_begin, scores, allowed = block_scores(block_id)
            masked = jnp.where(allowed, scores, MASK_FLOOR)
            new_peak = jnp.maximum(row_peak, jnp.max(masked, axis=2))
            new_mass = row_mass * jnp.exp(row_peak - new_peak) + jnp.sum(
                jnp.where(allowed, jnp.exp(masked - new_peak[:, :, None]), 0.0), axis=2
            )
            return (new_peak, new_mass)

        return (gated(block_id, update, running), None)

    initial = (
        jnp.full((head_count, tok_dev), MASK_FLOOR, jnp.float32),
        jnp.zeros((head_count, tok_dev), jnp.float32),
    )
    (row_peak, row_mass), _ = lax.scan(stats_step, initial, block_ids)
    log_total = row_peak + jnp.log(row_mass)

    def value_step(running, block_id):

        def update(state):
            weighted, partials = state
            key_begin, scores, allowed = block_scores(block_id)
            weights = jnp.where(allowed, jnp.exp(scores - log_total[:, :, None]), 0.0).astype(
                jnp.bfloat16
            )
            value_rows = lax.dynamic_slice_in_dim(values_all, key_begin, key_span, 0).reshape(
                key_span, head_count, HEAD_DIM
            )
            weighted = weighted + jnp.einsum(
                "hqk,khd->qhd", weights, value_rows, preferred_element_type=jnp.float32
            )
            return (weighted, partials)

        return (gated(block_id, update, running), None)

    partial_rows = 8
    value_init = (
        jnp.zeros((tok_dev, head_count, HEAD_DIM), jnp.float32),
        jnp.zeros((partial_rows, row_width), jnp.float32),
    )
    (weighted, partials), _ = lax.scan(value_step, value_init, block_ids)
    attended = weighted.reshape(tok_dev, row_width).astype(jnp.bfloat16)
    stats_all = lax.all_gather(log_total.T, "tokens", axis=0, tiled=True)
    query_rows = lax.all_gather(query_in, "tokens", axis=0, tiled=True)
    grad_rows = lax.all_gather(out_grads, "tokens", axis=0, tiled=True)
    piece_rows = query_rows.shape[0]
    piece_pos = jnp.arange(piece_rows, dtype=jnp.int32)

    def update(grad_sum):
        scores, allowed = pair_scores(query_rows, key_in, piece_pos, query_pos, doc_starts)
        weights = jnp.where(allowed, jnp.exp(scores - stats_all.T[:, :, None]), 0.0).astype(
            jnp.bfloat16
        )
        piece_grads = grad_rows.reshape(piece_rows, head_count, HEAD_DIM)
        return jnp.einsum("hqk,qhd->khd", weights, piece_grads, preferred_element_type=jnp.float32)

    summed = update(jnp.zeros((tok_dev, head_count, HEAD_DIM), jnp.float32))
    value_grads = summed.reshape(tok_dev, row_width).astype(jnp.bfloat16)
    token_shards = lax.axis_size("tokens")
    col_shards = lax.axis_size("cols")
    rows_attended, rows_grads = (
        lax.all_gather(attended[None], ("tokens", "cols"), axis=0, tiled=True),
        lax.all_gather(value_grads[None], ("tokens", "cols"), axis=0, tiled=True),
    )
    rows_attended = rows_attended.reshape(token_shards, col_shards, tok_dev, row_width)
    rows_grads = rows_grads.reshape(token_shards, col_shards, tok_dev, row_width)
    own_attended = lax.dynamic_index_in_dim(
        rows_attended, lax.axis_index("cols"), 1, keepdims=False
    )
    own_grads = lax.dynamic_index_in_dim(rows_grads, lax.axis_index("cols"), 1, keepdims=False)
    cols_attended, cols_grads = (
        spread(own_attended, "heads", lax.axis_index("tokens")),
        spread(own_grads, "heads", lax.axis_index("tokens")),
    )
    input_factor = jnp.einsum(
        "acnf,ang->cfg", rows_attended, cols_attended, preferred_element_type=jnp.float32
    )
    grad_factor = jnp.einsum(
        "acnf,ang->cfg", rows_grads, cols_grads, preferred_element_type=jnp.float32
    )
    input_factor = input_factor.reshape(col_shards * row_width, row_width) / all_tokens
    grad_factor = grad_factor.reshape(col_shards * row_width, row_width) / all_tokens
    return (input_factor, grad_factor)


TO_END = ((1, 1, 0), (1, 1, 1))
QUERY, KEY, VALUE, GRAD = range(4)
MATE, ACROSS, END = range(3)
F32 = jnp.float32
BF16 = jnp.bfloat16


def fused_kernel(
    starts_ref, q_ref, k_ref, v_ref, g_ref, out_a, out_g,
    xin, rows, cols, v_t, g_acc, key_doc, query_doc,
    a2a_send, a2a_recv, row_recv, up_send, down_send, x_send, chunk_send, swap_send,
    col_recv, pair_send, y_send, relay_send,
):
    n = lax.axis_size("tokens")
    tok_dev = q_ref.shape[0]
    all_tokens = n * tok_dev
    h = lax.axis_index("heads")
    z = lax.axis_index("tokens")
    x = lax.axis_index("cols")
    y = h // 2
    core = h % 2
    other_x = 1 - x
    pair = y * 2 + (1 - core)
    inputs = (q_ref, k_ref, v_ref, g_ref)
    half = HEAD_DIM // 2
    sources = (z + 1 - 2 * (z % 2), 2 - z // 2, 3 - 3 * (z // 2))

    barrier = pltpu.get_barrier_semaphore()
    for step in range(1, n):
        pl.semaphore_signal(barrier, inc=1, device_id={"tokens": (z + step) % n})
    for step in range(1, 4):
        pl.semaphore_signal(barrier, inc=1, device_id={"heads": (h + step) % 4})
    pl.semaphore_signal(barrier, inc=1, device_id={"cols": other_x})
    pl.semaphore_wait(barrier, n + 3)

    def feature_block(j, a, target):
        return inputs[a].at[:, pl.ds(pl.multiple_of((j * n + target) * HEAD_DIM, HEAD_DIM), HEAD_DIM)]

    def token_block(j, a, source):
        return xin.at[j, a, pl.ds(pl.multiple_of(source * tok_dev, tok_dev), tok_dev), :]

    def own_copy(j, a):
        return pltpu.make_async_copy(
            feature_block(j, a, z), token_block(j, a, z), a2a_recv.at[j, a, z]
        )

    def a2a_copy(j, a, source):
        target = sources[source]
        return pltpu.make_async_remote_copy(
            src_ref=feature_block(j, a, target), dst_ref=token_block(j, a, z),
            send_sem=a2a_send.at[j, a, source], recv_sem=a2a_recv.at[j, a, z],
            device_id={"tokens": target},
        )

    def arrived(j, a, position):
        block = token_block(j, a, position)
        pltpu.make_async_copy(block, block, a2a_recv.at[j, a, position]).wait()

    middle = (z > 0) & (z < n - 1)
    mate = sources[MATE]

    def send_inputs(j, kinds, targets):
        for source in targets:
            for a in kinds:
                a2a_copy(j, a, source).start()

    def send_own(j, kinds):
        for a in kinds:
            own_copy(j, a).start()

    def send_far(j, kinds):
        @pl.when(middle)
        def _():
            send_inputs(j, kinds, (END, ACROSS))

        @pl.when(jnp.logical_not(middle))
        def _():
            send_inputs(j, kinds, (ACROSS, END))

    def send_next(kinds):
        @pl.when(jnp.logical_not(middle))
        def _():
            send_inputs(1, kinds, (MATE,))

        send_far(1, kinds)

    def chunk_copy(position):
        piece = rows.at[0, 0, x, z, :, token_span(position)]
        return pltpu.make_async_remote_copy(
            src_ref=piece, dst_ref=piece, send_sem=chunk_send.at[position],
            recv_sem=row_recv.at[0, 0, x, z, 0], device_id={"cols": other_x},
        )

    def token_span(position):
        return pl.ds(pl.multiple_of(position * tok_dev, tok_dev), tok_dev)

    def attention(j, before, after):
        for position in (z,) + sources:
            arrived(j, VALUE, position)
        v_t[...] = xin[j, VALUE].astype(F32).T.astype(BF16)
        g_acc[...] = jnp.zeros_like(g_acc)

        def step(i, carry):
            far_first = (i == 2) == middle
            position = jnp.where(i == 0, z, jnp.where(i == 1, mate, jnp.where(far_first, sources[END], sources[ACROSS])))

            @pl.when(i == 2)
            def _():
                before()

            arrived(j, QUERY, position)
            arrived(j, GRAD, position)

            @pl.when(i == 2)
            def _():
                after()

            attention_block(j, position)
            if j == 0:
                chunk_copy(position).start()
            return carry

        lax.fori_loop(0, n, step, 0)
        rows[j, 1, x, z] = g_acc[...].T.astype(BF16)

    def attention_block(j, position):
        span = token_span(position)
        s = lax.dot_general(
            xin[j, KEY], xin[j, QUERY, span, :], (((1,), (1,)), ((), ())),
            preferred_element_type=F32,
        ) * (1.0 / math.sqrt(HEAD_DIM))
        s = jnp.where(key_doc[...] == query_doc[:, span], s, MASK_FLOOR)
        e = jnp.exp(s - jnp.max(s, axis=0, keepdims=True))
        p = (e * (1.0 / jnp.sum(e, axis=0, keepdims=True))).astype(BF16)
        att = jnp.dot(v_t[...], p, preferred_element_type=F32)
        rows[j, 0, x, z, :, span] = att.astype(BF16)
        g_acc[...] += jnp.dot(p, xin[j, GRAD, span, :], preferred_element_type=F32)

    def row_copy(j, f, xs, zs, part, send, device):
        piece = rows.at[j, f, xs, zs, pl.ds(part * half, half), :]
        return pltpu.make_async_remote_copy(
            src_ref=piece, dst_ref=piece, send_sem=send,
            recv_sem=row_recv.at[j, f, xs, zs, part], device_id=device,
        )

    over_x = {"cols": other_x}

    def up_copy(j, f, part, zs):
        return row_copy(j, f, x, zs, part, up_send.at[j, f, part, zs], {"tokens": (z + 1) % n})

    def down_copy(j, f, part, zs):
        return row_copy(j, f, x, zs, part, down_send.at[j, f, part, zs], {"tokens": (z + n - 1) % n})

    def x_copy(j, f, part, zs):
        return row_copy(j, f, x, zs, part, x_send.at[j, f, part, zs], over_x)

    def swap_copy(j, f, part):
        return row_copy(j, f, other_x, z, part, swap_send.at[j, f, part], {"tokens": mate})

    def own_rows(j, f, later=False):
        for part in range(2):
            @pl.when((z < n - 1) & (z != n // 2 - 1) if later else z < n - 1)
            def _():
                up_copy(j, f, part, z).start()

            @pl.when((z > 0) & (z != n // 2) if later else z > 0)
            def _():
                down_copy(j, f, part, z).start()

            if (j, f) != (0, 0):
                x_copy(j, f, part, z).start()
        feed_cols(j, f, z)

    def own_inward(j, f):
        for part in range(2):
            @pl.when(z == n // 2 - 1)
            def _():
                up_copy(j, f, part, z).start()

            @pl.when(z == n // 2)
            def _():
                down_copy(j, f, part, z).start()

    def rows_in(j, f, source):
        zs = sources[source]
        for part in range(2):
            x_copy(j, f, part, zs).wait_recv()

            @pl.when((zs < z) & (z < n - 1))
            def _():
                up_copy(j, f, part, zs).start()

            @pl.when((zs > z) & (z > 0))
            def _():
                down_copy(j, f, part, zs).start()

            if source != MATE:
                x_copy(j, f, part, zs).start()
            elif (j, f, part) not in TO_END:
                @pl.when(jnp.logical_not(middle))
                def _():
                    x_copy(j, f, part, zs).start()
        feed_cols(j, f, zs)

    def other_in(j, f, source, part):
        zs = z if source is None else sources[source]
        if (j, f, source) == (0, 0, None):
            if part == 0:
                piece = rows.at[0, 0, other_x, z]
                pltpu.make_async_copy(piece, piece, row_recv.at[0, 0, other_x, z, 0]).wait()
            return
        row_copy(j, f, other_x, zs, part, x_send.at[j, f, part, zs], over_x).wait_recv()

    def swap_rows(j, f, parts):
        for part in parts:
            other_in(j, f, None, part)
        for part in parts:
            swap_copy(j, f, part).start()

    def swap_to_end():
        for j, f, part in TO_END:
            swap_rows(j, f, (part,))

    def other_rows(j, f, group):
        if group == (MATE,):
            for part in range(2):
                if (j, f, part) not in TO_END:
                    @pl.when(middle)
                    def _():
                        other_in(j, f, None, part)
        for source in group:
            for part in range(2):
                other_in(j, f, source, part)

    is_source = h == z
    far = y != z // 2

    def col_copy(j, f, zs, source, send, device):
        return pltpu.make_async_remote_copy(
            src_ref=source, dst_ref=cols.at[j, f, zs], send_sem=send.at[j, f, zs],
            recv_sem=col_recv.at[j, f, zs], device_id={"heads": device},
        )

    def pair_copy(j, f, zs):
        return col_copy(j, f, zs, rows.at[j, f, x, zs], pair_send, pair)

    def y_copy(j, f, zs):
        return col_copy(j, f, zs, rows.at[j, f, x, zs], y_send, (1 - y) * 2 + zs % 2)

    def relay_copy(j, f, zs):
        return col_copy(j, f, zs, cols.at[j, f, zs], relay_send, pair)

    def feed_cols(j, f, zs):
        @pl.when(is_source)
        def _():
            y_copy(j, f, zs).start()
            pair_copy(j, f, zs).start()

    def relay_cols(j, f, source):
        zs = z if source is None else sources[source]

        @pl.when(far & (core == zs % 2))
        def _():
            relay_copy(j, f, zs).wait_recv()
            relay_copy(j, f, zs).start()

    def cols_in(j, f, source):
        zs = z if source is None else sources[source]

        @pl.when(jnp.logical_not(is_source | (far & (core == zs % 2))))
        def _():
            relay_copy(j, f, zs).wait_recv()

        @pl.when(is_source)
        def _():
            cols[j, f, zs] = rows[j, f, x, zs]

    wide = 2 * HEAD_DIM

    def products(f, xs, left, right):
        count = len(left) * len(right)

        def one(i, carry):
            at_left, at_right = i // len(right), i % len(right)
            jr = sum(((at_left == k) * item[0] for k, item in enumerate(left)), 0)
            pr = sum(((at_left == k) * item[1] for k, item in enumerate(left)), 0)
            jc = sum(((at_right == k) * item[0] for k, item in enumerate(right)), 0)
            pc = sum(((at_right == k) * item[1] for k, item in enumerate(right)), 0)
            row = pl.multiple_of((4 * xs + 2 * jr + pr) * wide, wide)
            col = pl.multiple_of((2 * jc + pc) * wide, wide)
            (out_a, out_g)[f][pl.ds(row, wide), pl.ds(col, wide)] = lax.dot_general(
                rows[jr, f, xs, pl.ds(2 * pr, 2)].reshape(wide, all_tokens),
                cols[jc, f, pl.ds(2 * pc, 2)].reshape(wide, all_tokens),
                (((1,), (1,)), ((), ())), preferred_element_type=F32,
            ) * (1.0 / all_tokens)
            return carry

        lax.fori_loop(0, count, one, 0)

    for a in (KEY, VALUE):
        send_inputs(0, (a,), (END, ACROSS))
    send_inputs(0, (KEY, VALUE), (MATE,))
    send_own(0, (KEY, VALUE, QUERY, GRAD))
    send_own(1, (KEY, VALUE, QUERY, GRAD))
    doc_count = starts_ref.shape[0]
    key_pos = lax.broadcasted_iota(jnp.int32, key_doc.shape, 0)
    query_pos = lax.broadcasted_iota(jnp.int32, query_doc.shape, 1)
    key_doc[...] = sum((key_pos >= starts_ref[d]).astype(jnp.int32) for d in range(doc_count))
    query_doc[...] = sum((query_pos >= starts_ref[d]).astype(jnp.int32) for d in range(doc_count))
    for position in (z,) + sources:
        arrived(0, KEY, position)
    send_inputs(0, (QUERY, GRAD), (MATE,))
    send_far(0, (QUERY, GRAD))

    @pl.when(middle)
    def _():
        send_inputs(1, (KEY, VALUE, QUERY, GRAD), (MATE,))

    def nothing():
        pass

    def send_rest():
        send_next((KEY, VALUE))
        send_next((QUERY, GRAD))

    def at_ends(j, f):
        @pl.when(jnp.logical_not(middle))
        def _():
            rows_in(j, f, MATE)

    def in_middle(j, f):
        @pl.when(middle)
        def _():
            rows_in(j, f, MATE)

    def end_swap(j, f):
        @pl.when(jnp.logical_not(middle))
        def _():
            swap_rows(j, f, range(2))

    attention(0, nothing, send_rest)
    own_rows(0, 0)
    own_rows(0, 1)
    at_ends(0, 0)
    for position in (z,) + sources:
        arrived(1, KEY, position)

    def gather_middle():
        in_middle(0, 0)

    def relay_pair(j, f, group):
        for source in group:
            relay_cols(j, f, source)

    def cols_pair(j, f, group):
        for source in group:
            cols_in(j, f, source)

    attention(1, lambda: at_ends(0, 1), gather_middle)
    near = z // 2
    first, last = (0, near), (0, 1 - near)
    second, final = (1, near), (1, 1 - near)
    own_rows(1, 0)
    own_rows(1, 1, later=True)
    in_middle(0, 1)
    at_ends(1, 0)
    end_swap(0, 0)
    end_swap(0, 1)
    at_ends(1, 1)
    rows_in(0, 0, ACROSS)
    in_middle(1, 0)
    own_inward(1, 1)
    end_swap(1, 0)
    rows_in(0, 1, ACROSS)
    in_middle(1, 1)
    end_swap(1, 1)
    relay_pair(0, 0, (None, MATE))
    relay_pair(0, 1, (None, MATE))
    rows_in(0, 0, END)
    relay_pair(1, 0, (None, MATE))
    relay_pair(1, 1, (None,))
    cols_pair(0, 0, (None, MATE))
    cols_pair(1, 0, (None, MATE))
    products(0, x, (first, second), (first, second))
    rows_in(1, 0, ACROSS)
    relay_pair(0, 0, (ACROSS,))
    relay_pair(0, 1, (ACROSS,))
    relay_pair(1, 1, (MATE,))
    cols_pair(0, 1, (None, MATE))
    cols_pair(1, 1, (None, MATE))
    products(1, x, (first, second), (first, second))
    rows_in(0, 1, END)
    relay_pair(0, 0, (END,))
    cols_pair(0, 0, (ACROSS, END))
    products(0, x, (last,), (first, second, last))
    products(0, x, (first, second), (last,))
    relay_pair(1, 0, (ACROSS,))
    rows_in(1, 0, END)
    relay_pair(0, 1, (END,))
    other_rows(0, 0, (MATE,))
    other_rows(1, 0, (MATE,))
    products(0, other_x, (first, second), (first, second, last))
    cols_pair(0, 1, (ACROSS, END))
    products(1, x, (last,), (first, second, last))
    products(1, x, (first, second), (last,))
    rows_in(1, 1, ACROSS)
    relay_pair(1, 0, (END,))
    other_rows(0, 1, (MATE,))
    products(1, other_x, (first,), (first, second, last))
    cols_pair(1, 0, (ACROSS, END))
    products(0, x, (final,), (first, second, last, final))
    products(0, x, (first, second, last), (final,))
    products(0, other_x, (first, second), (final,))
    other_rows(0, 0, (ACROSS, END))
    products(0, other_x, (last,), (first, second, last, final))
    other_rows(0, 1, (ACROSS, END))
    products(1, other_x, (last,), (first, second, last))
    rows_in(1, 1, END)

    @pl.when(middle)
    def _():
        swap_to_end()

    relay_pair(1, 1, (ACROSS,))
    products(1, x, (final,), (first, second, last))
    relay_pair(1, 1, (END,))
    other_rows(1, 0, (ACROSS, END))
    products(0, other_x, (final,), (first, second, last, final))
    cols_pair(1, 1, (ACROSS, END))
    products(1, x, (first, second, last, final), (final,))
    products(1, other_x, (first, last), (final,))
    other_rows(1, 1, (MATE,))
    products(1, other_x, (second,), (first, second, last, final))
    other_rows(1, 1, (ACROSS, END))
    products(1, other_x, (final,), (first, second, last, final))
    for j in range(2):
        for a in range(4):
            for source in range(3):
                a2a_copy(j, a, source).wait_send()
        for f in range(2):
            for part in range(2):
                def sent(zs, carry):
                    own_chunks = (zs == z) if (j, f) == (0, 0) else False
                    swapped = (zs == mate) if (j, f, part) in TO_END else (zs == mate) & middle

                    @pl.when(jnp.logical_not(swapped | own_chunks))
                    def _():
                        x_copy(j, f, part, zs).wait_send()

                    if (j, f, part) == (0, 0, 0):
                        chunk_copy(zs).wait_send()

                    @pl.when((z < n - 1) & (zs <= z))
                    def _():
                        up_copy(j, f, part, zs).wait_send()

                    @pl.when((z > 0) & (zs >= z))
                    def _():
                        down_copy(j, f, part, zs).wait_send()

                    return carry

                lax.fori_loop(0, n, sent, 0)
            for zs in range(n):
                @pl.when(is_source)
                def _():
                    pair_copy(j, f, zs).wait_send()
                    y_copy(j, f, zs).wait_send()

                @pl.when(far & (core == zs % 2))
                def _():
                    relay_copy(j, f, zs).wait_send()
    for j in range(2):
        for f in range(2):
            for part in range(2):
                if (j, f, part) in TO_END:
                    swap_copy(j, f, part).wait_send()
                else:
                    @pl.when(jnp.logical_not(middle))
                    def _():
                        swap_copy(j, f, part).wait_send()


def fused(query_in, key_in, value_in, out_grads, doc_starts):
    n = lax.axis_size("tokens")
    tok_dev, row_width = query_in.shape
    all_tokens = n * tok_dev
    dma = pltpu.SemaphoreType.DMA
    hbm = pl.BlockSpec(memory_space=pl.ANY)
    smem = pl.BlockSpec(memory_space=pltpu.SMEM)
    out = pltpu.VMEM((2 * row_width, row_width), F32)
    return tuple(pl.pallas_call(
        fused_kernel,
        out_shape=(out, out),
        in_specs=[smem] + [hbm] * 4,
        out_specs=[pl.BlockSpec(memory_space=pltpu.VMEM)] * 2,
        scratch_shapes=[
            pltpu.VMEM((2, 4, all_tokens, HEAD_DIM), BF16),
            pltpu.VMEM((2, 2, 2, n, HEAD_DIM, all_tokens), BF16),
            pltpu.VMEM((2, 2, n, HEAD_DIM, all_tokens), BF16),
            pltpu.VMEM((HEAD_DIM, all_tokens), BF16),
            pltpu.VMEM((all_tokens, HEAD_DIM), F32),
            pltpu.VMEM((all_tokens, 1), jnp.int32),
            pltpu.VMEM((1, all_tokens), jnp.int32),
            dma((2, 4, 3)), dma((2, 4, n)), dma((2, 2, 2, n, 2)),
            dma((2, 2, 2, n)), dma((2, 2, 2, n)), dma((2, 2, 2, n)), dma((n,)), dma((2, 2, 2)),
            dma((2, 2, n)), dma((2, 2, n)), dma((2, 2, n)), dma((2, 2, n)),
        ],
        compiler_params=pltpu.CompilerParams(
            collective_id=0, has_side_effects=True, vmem_limit_bytes=38 * 1024 * 1024
        ),
    )(doc_starts, query_in, key_in, value_in, out_grads))


def per_device(query_in, key_in, value_in, out_grads, doc_starts):
    n = lax.axis_size("tokens")
    fits = n == 4 and lax.axis_size("heads") == 4 and lax.axis_size("cols") == 2
    if fits and query_in.shape[1] == 2 * n * HEAD_DIM and query_in.shape[0] % HEAD_DIM == 0:
        return fused(query_in, key_in, value_in, out_grads, doc_starts)
    return on_device(query_in, key_in, value_in, out_grads, doc_starts)


def solution(mesh):
    in_specs = (
        P("tokens", ("heads", "cols")),
        P("tokens", ("heads", "cols")),
        P("tokens", ("heads", "cols")),
        P("tokens", ("heads", "cols")),
        P(),
    )
    out_specs = (P("heads", ("tokens", "cols")), P("heads", ("tokens", "cols")))
    return jax.shard_map(
        per_device, mesh=mesh, in_specs=in_specs, out_specs=out_specs, check_vma=False
    )
```

```python
import math

import jax
import jax.numpy as jnp
from jax import lax
from jax.experimental import pallas as pl
from jax.experimental.pallas import tpu as pltpu
from jax.sharding import PartitionSpec as P

HEAD_DIM = 128


MASK_FLOOR = -1e30


def spread(value, axis, source):
    kept = jnp.where(lax.axis_index(axis) == source, value, 0).astype(value.dtype)
    return lax.psum(kept, axis)


def document_ids(positions, doc_starts):
    return jnp.sum((positions[:, None] >= doc_starts[None, :]).astype(jnp.int32), axis=1) - 1


def pair_scores(query_rows, key_rows, query_pos, key_pos, doc_starts):
    head_count = query_rows.shape[1] // HEAD_DIM
    query_heads = query_rows.reshape(query_rows.shape[0], head_count, HEAD_DIM)
    key_heads = key_rows.reshape(key_rows.shape[0], head_count, HEAD_DIM)
    scores = jnp.einsum(
        "qhd,khd->hqk", query_heads, key_heads, preferred_element_type=jnp.float32
    ) * (1.0 / math.sqrt(HEAD_DIM))
    query_docs = document_ids(query_pos, doc_starts)
    key_docs = document_ids(key_pos, doc_starts)
    allowed = query_docs[:, None] == key_docs[None, :]
    return (scores, allowed[None, :, :])


def on_device(query_in, key_in, value_in, out_grads, doc_starts):
    tok_dev, row_width = query_in.shape
    head_count = row_width // HEAD_DIM
    first_pos = lax.axis_index("tokens") * tok_dev
    query_pos = first_pos + jnp.arange(tok_dev, dtype=jnp.int32)
    keys_all, values_all = (
        lax.all_gather(key_in, "tokens", axis=0, tiled=True),
        lax.all_gather(value_in, "tokens", axis=0, tiled=True),
    )
    all_tokens = keys_all.shape[0]
    key_span = min(512, all_tokens)
    block_ids = jnp.arange(all_tokens // key_span, dtype=jnp.int32)

    def block_scores(block_id):
        key_begin = block_id * key_span
        key_rows = lax.dynamic_slice_in_dim(keys_all, key_begin, key_span, 0)
        key_pos = key_begin + jnp.arange(key_span, dtype=jnp.int32)
        scores, allowed = pair_scores(query_in, key_rows, query_pos, key_pos, doc_starts)
        return (key_begin, scores, allowed)

    def gated(block_id, update, running):
        key_begin = block_id * key_span
        return update(running)

    def stats_step(running, block_id):

        def update(state):
            row_peak, row_mass = state
            key_begin, scores, allowed = block_scores(block_id)
            masked = jnp.where(allowed, scores, MASK_FLOOR)
            new_peak = jnp.maximum(row_peak, jnp.max(masked, axis=2))
            new_mass = row_mass * jnp.exp(row_peak - new_peak) + jnp.sum(
                jnp.where(allowed, jnp.exp(masked - new_peak[:, :, None]), 0.0), axis=2
            )
            return (new_peak, new_mass)

        return (gated(block_id, update, running), None)

    initial = (
        jnp.full((head_count, tok_dev), MASK_FLOOR, jnp.float32),
        jnp.zeros((head_count, tok_dev), jnp.float32),
    )
    (row_peak, row_mass), _ = lax.scan(stats_step, initial, block_ids)
    log_total = row_peak + jnp.log(row_mass)

    def value_step(running, block_id):

        def update(state):
            weighted, partials = state
            key_begin, scores, allowed = block_scores(block_id)
            weights = jnp.where(allowed, jnp.exp(scores - log_total[:, :, None]), 0.0).astype(
                jnp.bfloat16
            )
            value_rows = lax.dynamic_slice_in_dim(values_all, key_begin, key_span, 0).reshape(
                key_span, head_count, HEAD_DIM
            )
            weighted = weighted + jnp.einsum(
                "hqk,khd->qhd", weights, value_rows, preferred_element_type=jnp.float32
            )
            return (weighted, partials)

        return (gated(block_id, update, running), None)

    partial_rows = 8
    value_init = (
        jnp.zeros((tok_dev, head_count, HEAD_DIM), jnp.float32),
        jnp.zeros((partial_rows, row_width), jnp.float32),
    )
    (weighted, partials), _ = lax.scan(value_step, value_init, block_ids)
    attended = weighted.reshape(tok_dev, row_width).astype(jnp.bfloat16)
    stats_all = lax.all_gather(log_total.T, "tokens", axis=0, tiled=True)
    query_rows = lax.all_gather(query_in, "tokens", axis=0, tiled=True)
    grad_rows = lax.all_gather(out_grads, "tokens", axis=0, tiled=True)
    piece_rows = query_rows.shape[0]
    piece_pos = jnp.arange(piece_rows, dtype=jnp.int32)

    def update(grad_sum):
        scores, allowed = pair_scores(query_rows, key_in, piece_pos, query_pos, doc_starts)
        weights = jnp.where(allowed, jnp.exp(scores - stats_all.T[:, :, None]), 0.0).astype(
            jnp.bfloat16
        )
        piece_grads = grad_rows.reshape(piece_rows, head_count, HEAD_DIM)
        return jnp.einsum("hqk,qhd->khd", weights, piece_grads, preferred_element_type=jnp.float32)

    summed = update(jnp.zeros((tok_dev, head_count, HEAD_DIM), jnp.float32))
    value_grads = summed.reshape(tok_dev, row_width).astype(jnp.bfloat16)
    token_shards = lax.axis_size("tokens")
    col_shards = lax.axis_size("cols")
    rows_attended, rows_grads = (
        lax.all_gather(attended[None], ("tokens", "cols"), axis=0, tiled=True),
        lax.all_gather(value_grads[None], ("tokens", "cols"), axis=0, tiled=True),
    )
    rows_attended = rows_attended.reshape(token_shards, col_shards, tok_dev, row_width)
    rows_grads = rows_grads.reshape(token_shards, col_shards, tok_dev, row_width)
    own_attended = lax.dynamic_index_in_dim(
        rows_attended, lax.axis_index("cols"), 1, keepdims=False
    )
    own_grads = lax.dynamic_index_in_dim(rows_grads, lax.axis_index("cols"), 1, keepdims=False)
    cols_attended, cols_grads = (
        spread(own_attended, "heads", lax.axis_index("tokens")),
        spread(own_grads, "heads", lax.axis_index("tokens")),
    )
    input_factor = jnp.einsum(
        "acnf,ang->cfg", rows_attended, cols_attended, preferred_element_type=jnp.float32
    )
    grad_factor = jnp.einsum(
        "acnf,ang->cfg", rows_grads, cols_grads, preferred_element_type=jnp.float32
    )
    input_factor = input_factor.reshape(col_shards * row_width, row_width) / all_tokens
    grad_factor = grad_factor.reshape(col_shards * row_width, row_width) / all_tokens
    return (input_factor, grad_factor)


TO_END = ((1, 1, 0), (1, 1, 1))
QUERY, KEY, VALUE, GRAD = range(4)
MATE, ACROSS, END = range(3)
F32 = jnp.float32
BF16 = jnp.bfloat16


def fused_kernel(
    starts_ref, q_ref, k_ref, v_ref, g_ref, out_a, out_g,
    xin, rows, cols, v_t, g_acc, key_doc, query_doc,
    a2a_send, a2a_recv, row_recv, up_send, down_send, x_send, chunk_send, swap_send,
    col_recv, pair_send, y_send, relay_send,
):
    n = lax.axis_size("tokens")
    tok_dev = q_ref.shape[0]
    all_tokens = n * tok_dev
    h = lax.axis_index("heads")
    z = lax.axis_index("tokens")
    x = lax.axis_index("cols")
    y = h // 2
    core = h % 2
    other_x = 1 - x
    pair = y * 2 + (1 - core)
    inputs = (q_ref, k_ref, v_ref, g_ref)
    half = HEAD_DIM // 2
    sources = (z + 1 - 2 * (z % 2), 2 - z // 2, 3 - 3 * (z // 2))

    barrier = pltpu.get_barrier_semaphore()
    for step in range(1, n):
        pl.semaphore_signal(barrier, inc=1, device_id={"tokens": (z + step) % n})
    for step in range(1, 4):
        pl.semaphore_signal(barrier, inc=1, device_id={"heads": (h + step) % 4})
    pl.semaphore_signal(barrier, inc=1, device_id={"cols": other_x})
    pl.semaphore_wait(barrier, n + 3)

    def feature_block(j, a, target):
        return inputs[a].at[:, pl.ds(pl.multiple_of((j * n + target) * HEAD_DIM, HEAD_DIM), HEAD_DIM)]

    def token_block(j, a, source):
        return xin.at[j, a, pl.ds(pl.multiple_of(source * tok_dev, tok_dev), tok_dev), :]

    def own_copy(j, a):
        return pltpu.make_async_copy(
            feature_block(j, a, z), token_block(j, a, z), a2a_recv.at[j, a, z]
        )

    def a2a_copy(j, a, source):
        target = sources[source]
        return pltpu.make_async_remote_copy(
            src_ref=feature_block(j, a, target), dst_ref=token_block(j, a, z),
            send_sem=a2a_send.at[j, a, source], recv_sem=a2a_recv.at[j, a, z],
            device_id={"tokens": target},
        )

    def arrived(j, a, position):
        block = token_block(j, a, position)
        pltpu.make_async_copy(block, block, a2a_recv.at[j, a, position]).wait()

    middle = (z > 0) & (z < n - 1)
    mate = sources[MATE]

    def send_inputs(j, kinds, targets):
        for source in targets:
            for a in kinds:
                a2a_copy(j, a, source).start()

    def send_own(j, kinds):
        for a in kinds:
            own_copy(j, a).start()

    def send_far(j, kinds):
        @pl.when(middle)
        def _():
            send_inputs(j, kinds, (END, ACROSS))

        @pl.when(jnp.logical_not(middle))
        def _():
            send_inputs(j, kinds, (ACROSS, END))

    def send_next(kinds):
        @pl.when(jnp.logical_not(middle))
        def _():
            send_inputs(1, kinds, (MATE,))

        send_far(1, kinds)

    def chunk_copy(position):
        piece = rows.at[0, 0, x, z, :, token_span(position)]
        return pltpu.make_async_remote_copy(
            src_ref=piece, dst_ref=piece, send_sem=chunk_send.at[position],
            recv_sem=row_recv.at[0, 0, x, z, 0], device_id={"cols": other_x},
        )

    def token_span(position):
        return pl.ds(pl.multiple_of(position * tok_dev, tok_dev), tok_dev)

    def attention(j, before, after):
        for position in (z,) + sources:
            arrived(j, VALUE, position)
        v_t[...] = xin[j, VALUE].astype(F32).T.astype(BF16)
        g_acc[...] = jnp.zeros_like(g_acc)

        def step(i, carry):
            far_first = (i == 2) == middle
            position = jnp.where(i == 0, z, jnp.where(i == 1, mate, jnp.where(far_first, sources[END], sources[ACROSS])))

            @pl.when(i == 2)
            def _():
                before()

            arrived(j, QUERY, position)
            arrived(j, GRAD, position)

            @pl.when(i == 2)
            def _():
                after()

            attention_block(j, position)
            if j == 0:
                chunk_copy(position).start()
            return carry

        lax.fori_loop(0, n, step, 0)
        rows[j, 1, x, z] = g_acc[...].T.astype(BF16)

    def attention_block(j, position):
        span = token_span(position)
        s = lax.dot_general(
            xin[j, KEY], xin[j, QUERY, span, :], (((1,), (1,)), ((), ())),
            preferred_element_type=F32,
        ) * (1.0 / math.sqrt(HEAD_DIM))
        s = jnp.where(key_doc[...] == query_doc[:, span], s, MASK_FLOOR)
        e = jnp.exp(s - jnp.max(s, axis=0, keepdims=True))
        p = (e * (1.0 / jnp.sum(e, axis=0, keepdims=True))).astype(BF16)
        att = jnp.dot(v_t[...], p, preferred_element_type=F32)
        rows[j, 0, x, z, :, span] = att.astype(BF16)
        g_acc[...] += jnp.dot(p, xin[j, GRAD, span, :], preferred_element_type=F32)

    def row_copy(j, f, xs, zs, part, send, device):
        piece = rows.at[j, f, xs, zs, pl.ds(part * half, half), :]
        return pltpu.make_async_remote_copy(
            src_ref=piece, dst_ref=piece, send_sem=send,
            recv_sem=row_recv.at[j, f, xs, zs, part], device_id=device,
        )

    over_x = {"cols": other_x}

    def up_copy(j, f, part, zs):
        return row_copy(j, f, x, zs, part, up_send.at[j, f, part, zs], {"tokens": (z + 1) % n})

    def down_copy(j, f, part, zs):
        return row_copy(j, f, x, zs, part, down_send.at[j, f, part, zs], {"tokens": (z + n - 1) % n})

    def x_copy(j, f, part, zs):
        return row_copy(j, f, x, zs, part, x_send.at[j, f, part, zs], over_x)

    def swap_copy(j, f, part):
        return row_copy(j, f, other_x, z, part, swap_send.at[j, f, part], {"tokens": mate})

    def own_rows(j, f, later=False):
        for part in range(2):
            @pl.when((z < n - 1) & (z != n // 2 - 1) if later else z < n - 1)
            def _():
                up_copy(j, f, part, z).start()

            @pl.when((z > 0) & (z != n // 2) if later else z > 0)
            def _():
                down_copy(j, f, part, z).start()

            if (j, f) != (0, 0):
                x_copy(j, f, part, z).start()
            feed_cols(j, f, z, part)

    def own_inward(j, f):
        for part in range(2):
            @pl.when(z == n // 2 - 1)
            def _():
                up_copy(j, f, part, z).start()

            @pl.when(z == n // 2)
            def _():
                down_copy(j, f, part, z).start()

    def rows_in(j, f, source):
        zs = sources[source]
        for part in range(2):
            x_copy(j, f, part, zs).wait_recv()

            @pl.when((zs < z) & (z < n - 1))
            def _():
                up_copy(j, f, part, zs).start()

            @pl.when((zs > z) & (z > 0))
            def _():
                down_copy(j, f, part, zs).start()

            if source != MATE:
                x_copy(j, f, part, zs).start()
            elif (j, f, part) not in TO_END:
                @pl.when(jnp.logical_not(middle))
                def _():
                    x_copy(j, f, part, zs).start()
            feed_cols(j, f, zs, part)

    def other_in(j, f, source, part):
        zs = z if source is None else sources[source]
        if (j, f, source) == (0, 0, None):
            if part == 0:
                piece = rows.at[0, 0, other_x, z]
                pltpu.make_async_copy(piece, piece, row_recv.at[0, 0, other_x, z, 0]).wait()
            return
        row_copy(j, f, other_x, zs, part, x_send.at[j, f, part, zs], over_x).wait_recv()

    def swap_rows(j, f, parts):
        for part in parts:
            other_in(j, f, None, part)
        for part in parts:
            swap_copy(j, f, part).start()

    def swap_to_end():
        for j, f, part in TO_END:
            swap_rows(j, f, (part,))

    def other_rows(j, f, group):
        if group == (MATE,):
            for part in range(2):
                if (j, f, part) not in TO_END:
                    @pl.when(middle)
                    def _():
                        other_in(j, f, None, part)
        for source in group:
            for part in range(2):
                other_in(j, f, source, part)

    is_source = h == z
    far = y != z // 2

    def col_copy(j, f, zs, part, source, send, device):
        span = pl.ds(part * half, half)
        return pltpu.make_async_remote_copy(
            src_ref=source.at[span, :], dst_ref=cols.at[j, f, zs, span, :],
            send_sem=send.at[j, f, zs, part], recv_sem=col_recv.at[j, f, zs, part],
            device_id={"heads": device},
        )

    def pair_copy(j, f, zs, part):
        return col_copy(j, f, zs, part, rows.at[j, f, x, zs], pair_send, pair)

    def y_copy(j, f, zs, part):
        return col_copy(j, f, zs, part, rows.at[j, f, x, zs], y_send, (1 - y) * 2 + zs % 2)

    def relay_copy(j, f, zs, part):
        return col_copy(j, f, zs, part, cols.at[j, f, zs], relay_send, pair)

    def feed_cols(j, f, zs, part):
        @pl.when(is_source)
        def _():
            y_copy(j, f, zs, part).start()
            pair_copy(j, f, zs, part).start()

    def relay_cols(j, f, source):
        zs = z if source is None else sources[source]

        @pl.when(far & (core == zs % 2))
        def _():
            for part in range(2):
                relay_copy(j, f, zs, part).wait_recv()
                relay_copy(j, f, zs, part).start()

    def cols_in(j, f, source):
        zs = z if source is None else sources[source]

        @pl.when(jnp.logical_not(is_source | (far & (core == zs % 2))))
        def _():
            for part in range(2):
                relay_copy(j, f, zs, part).wait_recv()

        @pl.when(is_source)
        def _():
            cols[j, f, zs] = rows[j, f, x, zs]

    wide = 2 * HEAD_DIM

    def products(f, xs, left, right):
        count = len(left) * len(right)

        def one(i, carry):
            at_left, at_right = i // len(right), i % len(right)
            jr = sum(((at_left == k) * item[0] for k, item in enumerate(left)), 0)
            pr = sum(((at_left == k) * item[1] for k, item in enumerate(left)), 0)
            jc = sum(((at_right == k) * item[0] for k, item in enumerate(right)), 0)
            pc = sum(((at_right == k) * item[1] for k, item in enumerate(right)), 0)
            row = pl.multiple_of((4 * xs + 2 * jr + pr) * wide, wide)
            col = pl.multiple_of((2 * jc + pc) * wide, wide)
            (out_a, out_g)[f][pl.ds(row, wide), pl.ds(col, wide)] = lax.dot_general(
                rows[jr, f, xs, pl.ds(2 * pr, 2)].reshape(wide, all_tokens),
                cols[jc, f, pl.ds(2 * pc, 2)].reshape(wide, all_tokens),
                (((1,), (1,)), ((), ())), preferred_element_type=F32,
            ) * (1.0 / all_tokens)
            return carry

        lax.fori_loop(0, count, one, 0)

    for a in (KEY, VALUE):
        send_inputs(0, (a,), (END, ACROSS))
    send_inputs(0, (KEY, VALUE), (MATE,))
    send_own(0, (KEY, VALUE, QUERY, GRAD))
    send_own(1, (KEY, VALUE, QUERY, GRAD))
    doc_count = starts_ref.shape[0]
    key_pos = lax.broadcasted_iota(jnp.int32, key_doc.shape, 0)
    query_pos = lax.broadcasted_iota(jnp.int32, query_doc.shape, 1)
    key_doc[...] = sum((key_pos >= starts_ref[d]).astype(jnp.int32) for d in range(doc_count))
    query_doc[...] = sum((query_pos >= starts_ref[d]).astype(jnp.int32) for d in range(doc_count))
    for position in (z,) + sources:
        arrived(0, KEY, position)
    send_inputs(0, (QUERY, GRAD), (MATE,))
    send_far(0, (QUERY, GRAD))

    @pl.when(middle)
    def _():
        send_inputs(1, (KEY, VALUE, QUERY, GRAD), (MATE,))

    def nothing():
        pass

    def send_rest():
        send_next((KEY, VALUE))
        send_next((QUERY, GRAD))

    def at_ends(j, f):
        @pl.when(jnp.logical_not(middle))
        def _():
            rows_in(j, f, MATE)

    def in_middle(j, f):
        @pl.when(middle)
        def _():
            rows_in(j, f, MATE)

    def end_swap(j, f):
        @pl.when(jnp.logical_not(middle))
        def _():
            swap_rows(j, f, range(2))

    attention(0, nothing, send_rest)
    own_rows(0, 0)
    own_rows(0, 1)
    at_ends(0, 0)
    for position in (z,) + sources:
        arrived(1, KEY, position)

    def gather_middle():
        in_middle(0, 0)

    def relay_pair(j, f, group):
        for source in group:
            relay_cols(j, f, source)

    def cols_pair(j, f, group):
        for source in group:
            cols_in(j, f, source)

    attention(1, lambda: at_ends(0, 1), gather_middle)
    near = z // 2
    first, last = (0, near), (0, 1 - near)
    second, final = (1, near), (1, 1 - near)
    own_rows(1, 0)
    own_rows(1, 1, later=True)
    in_middle(0, 1)
    at_ends(1, 0)
    end_swap(0, 0)
    end_swap(0, 1)
    at_ends(1, 1)
    rows_in(0, 0, ACROSS)
    in_middle(1, 0)
    own_inward(1, 1)
    end_swap(1, 0)
    rows_in(0, 1, ACROSS)
    in_middle(1, 1)
    end_swap(1, 1)
    relay_pair(0, 0, (None, MATE))
    relay_pair(0, 1, (None, MATE))
    rows_in(0, 0, END)
    relay_pair(1, 0, (None, MATE))
    relay_pair(1, 1, (None,))
    cols_pair(0, 0, (None, MATE))
    cols_pair(1, 0, (None, MATE))
    products(0, x, (first, second), (first, second))
    rows_in(1, 0, ACROSS)
    relay_pair(0, 0, (ACROSS,))
    relay_pair(0, 1, (ACROSS,))
    relay_pair(1, 1, (MATE,))
    cols_pair(0, 1, (None, MATE))
    cols_pair(1, 1, (None, MATE))
    products(1, x, (first, second), (first, second))
    rows_in(0, 1, END)
    relay_pair(0, 0, (END,))
    cols_pair(0, 0, (ACROSS, END))
    products(0, x, (last,), (first, second, last))
    products(0, x, (first, second), (last,))
    relay_pair(1, 0, (ACROSS,))
    rows_in(1, 0, END)
    relay_pair(0, 1, (END,))
    other_rows(0, 0, (MATE,))
    other_rows(1, 0, (MATE,))
    products(0, other_x, (first, second), (first, second, last))
    cols_pair(0, 1, (ACROSS, END))
    products(1, x, (last,), (first, second, last))
    products(1, x, (first, second), (last,))
    rows_in(1, 1, ACROSS)
    relay_pair(1, 0, (END,))
    other_rows(0, 1, (MATE,))
    products(1, other_x, (first,), (first, second, last))
    cols_pair(1, 0, (ACROSS, END))
    products(0, x, (final,), (first, second, last, final))
    products(0, x, (first, second, last), (final,))
    products(0, other_x, (first, second), (final,))
    other_rows(0, 0, (ACROSS, END))
    products(0, other_x, (last,), (first, second, last, final))
    other_rows(0, 1, (ACROSS, END))
    products(1, other_x, (last,), (first, second, last))
    rows_in(1, 1, END)

    @pl.when(middle)
    def _():
        swap_to_end()

    relay_pair(1, 1, (ACROSS,))
    products(1, x, (final,), (first, second, last))
    relay_pair(1, 1, (END,))
    other_rows(1, 0, (ACROSS, END))
    products(0, other_x, (final,), (first, second, last, final))
    cols_pair(1, 1, (ACROSS, END))
    products(1, x, (first, second, last, final), (final,))
    products(1, other_x, (first, last), (final,))
    other_rows(1, 1, (MATE,))
    products(1, other_x, (second,), (first, second, last, final))
    other_rows(1, 1, (ACROSS, END))
    products(1, other_x, (final,), (first, second, last, final))
    for j in range(2):
        for a in range(4):
            for source in range(3):
                a2a_copy(j, a, source).wait_send()
        for f in range(2):
            for part in range(2):
                def sent(zs, carry):
                    own_chunks = (zs == z) if (j, f) == (0, 0) else False
                    swapped = (zs == mate) if (j, f, part) in TO_END else (zs == mate) & middle

                    @pl.when(jnp.logical_not(swapped | own_chunks))
                    def _():
                        x_copy(j, f, part, zs).wait_send()

                    if (j, f, part) == (0, 0, 0):
                        chunk_copy(zs).wait_send()

                    @pl.when((z < n - 1) & (zs <= z))
                    def _():
                        up_copy(j, f, part, zs).wait_send()

                    @pl.when((z > 0) & (zs >= z))
                    def _():
                        down_copy(j, f, part, zs).wait_send()

                    return carry

                lax.fori_loop(0, n, sent, 0)
            for zs in range(n):
                for part in range(2):
                    @pl.when(is_source)
                    def _():
                        pair_copy(j, f, zs, part).wait_send()
                        y_copy(j, f, zs, part).wait_send()

                    @pl.when(far & (core == zs % 2))
                    def _():
                        relay_copy(j, f, zs, part).wait_send()
    for j in range(2):
        for f in range(2):
            for part in range(2):
                if (j, f, part) in TO_END:
                    swap_copy(j, f, part).wait_send()
                else:
                    @pl.when(jnp.logical_not(middle))
                    def _():
                        swap_copy(j, f, part).wait_send()


WRITES = 8


def write_kernel(a_ref, g_ref, out_a, out_g, sem):
    rows = a_ref.shape[0] // WRITES
    copies = [
        pltpu.make_async_copy(
            source.at[pl.ds(k * rows, rows), :], target.at[pl.ds(k * rows, rows), :], sem.at[f, k]
        )
        for k in range(WRITES)
        for f, (source, target) in enumerate(((a_ref, out_a), (g_ref, out_g)))
    ]
    for copy in copies:
        copy.start()
    for copy in copies:
        copy.wait()


def fused(query_in, key_in, value_in, out_grads, doc_starts):
    n = lax.axis_size("tokens")
    tok_dev, row_width = query_in.shape
    all_tokens = n * tok_dev
    dma = pltpu.SemaphoreType.DMA
    hbm = pl.BlockSpec(memory_space=pl.ANY)
    smem = pl.BlockSpec(memory_space=pltpu.SMEM)
    out = pltpu.VMEM((2 * row_width, row_width), F32)
    factors = pl.pallas_call(
        fused_kernel,
        out_shape=(out, out),
        in_specs=[smem] + [hbm] * 4,
        out_specs=[pl.BlockSpec(memory_space=pltpu.VMEM)] * 2,
        scratch_shapes=[
            pltpu.VMEM((2, 4, all_tokens, HEAD_DIM), BF16),
            pltpu.VMEM((2, 2, 2, n, HEAD_DIM, all_tokens), BF16),
            pltpu.VMEM((2, 2, n, HEAD_DIM, all_tokens), BF16),
            pltpu.VMEM((HEAD_DIM, all_tokens), BF16),
            pltpu.VMEM((all_tokens, HEAD_DIM), F32),
            pltpu.VMEM((all_tokens, 1), jnp.int32),
            pltpu.VMEM((1, all_tokens), jnp.int32),
            dma((2, 4, 3)), dma((2, 4, n)), dma((2, 2, 2, n, 2)),
            dma((2, 2, 2, n)), dma((2, 2, 2, n)), dma((2, 2, 2, n)), dma((n,)), dma((2, 2, 2)),
            dma((2, 2, n, 2)), dma((2, 2, n, 2)), dma((2, 2, n, 2)), dma((2, 2, n, 2)),
        ],
        compiler_params=pltpu.CompilerParams(
            collective_id=0, has_side_effects=True, vmem_limit_bytes=38 * 1024 * 1024
        ),
    )(doc_starts, query_in, key_in, value_in, out_grads)
    final = jax.ShapeDtypeStruct((2 * row_width, row_width), F32)
    return tuple(pl.pallas_call(
        write_kernel,
        out_shape=(final, final),
        in_specs=[pl.BlockSpec(memory_space=pltpu.VMEM)] * 2,
        out_specs=[hbm] * 2,
        scratch_shapes=[dma((2, WRITES))],
        compiler_params=pltpu.CompilerParams(vmem_limit_bytes=20 * 1024 * 1024),
    )(*factors))


def per_device(query_in, key_in, value_in, out_grads, doc_starts):
    n = lax.axis_size("tokens")
    fits = n == 4 and lax.axis_size("heads") == 4 and lax.axis_size("cols") == 2
    if fits and query_in.shape[1] == 2 * n * HEAD_DIM and query_in.shape[0] % HEAD_DIM == 0:
        return fused(query_in, key_in, value_in, out_grads, doc_starts)
    return on_device(query_in, key_in, value_in, out_grads, doc_starts)


def solution(mesh):
    in_specs = (
        P("tokens", ("heads", "cols")),
        P("tokens", ("heads", "cols")),
        P("tokens", ("heads", "cols")),
        P("tokens", ("heads", "cols")),
        P(),
    )
    out_specs = (P("heads", ("tokens", "cols")), P("heads", ("tokens", "cols")))
    return jax.shard_map(
        per_device, mesh=mesh, in_specs=in_specs, out_specs=out_specs, check_vma=False
    )
```
